256 devices in a mesh: lat: 128 (over x, z, y), lev: 2 (over core).
Axes of the slice: x: 4, y: 4, z: 8, core: 2. Of those that a mesh axis runs over, the one named last changes fastest.
Arguments:
- fields: float32 [1280, 3, 16, 2560], P('lat', None, 'lev'), may hold values from 0.1 to 5
- lat_fraction: float32 [1280], P('lat'), may hold values from 0 to 1
- lon_fraction: float32 [1280], P('lat'), may hold values from 0 to 1
- lon_shift: int32 [1280], P('lat'), may hold values from 0 to 2559
- departure_row: int32 [1280], P('lat'), may hold values from 1 to 1277, as said below
- extents: int32 [128, 2], P('lat'), may hold values from 1 to 4
Outputs:
- advected: float32 [1280, 3, 16, 2560], P('lat', None, 'lev')
The draws below stay inside these ranges and needn't reach their ends.
Inputs may be any that keep to these rules, and one draw needn't show every extreme that they name: departure_row[r] lies within 39 rows of r.
All inputs are finite; a program needn't handle non-finite values.
Results may differ from the reference program's by a relative error of at most 0.0003.
Values sent between devices are 32-bit elements; how exact they have to be, the bound alone decides.
A program may use at most 128 MiB of HBM per device.

```python
import math
import jax
import jax.numpy as jnp
from jax import lax

ROWS = 10
LON = 2560
FIELDS = 3
REACH = 4
NLAT = 1280
LEV = 16
BANDS = 128


def band_phase(key):
    return jax.random.randint(jax.random.fold_in(key, 911), (), 0, 8 * ROWS)


def draw_fields(key, part):
    row_phase = band_phase(key)
    shifted_rows = (jnp.arange(NLAT, dtype=jnp.int32) + row_phase) % (8 * ROWS)
    row_angle = 2.0 * math.pi * shifted_rows.astype(jnp.float32) / (8 * ROWS)
    full_shape = (NLAT, FIELDS, LEV, LON)
    gain_row = jnp.exp(-0.5 * jnp.sin(row_angle))
    rough_part = jax.random.uniform(jax.random.fold_in(key, 23), full_shape, jnp.float32, 0.5, 2.0)
    return (gain_row[:, None, None, None] * rough_part).astype(jnp.float32)


def draw_departure_row(key, part):
    row_phase = band_phase(key)
    row_ids = jnp.arange(NLAT, dtype=jnp.int32)
    shifted_rows = (row_ids + row_phase) % (8 * ROWS)
    row_drift = jnp.clip(2 * (2 * ROWS - jnp.abs(shifted_rows - 4 * ROWS)), -2 * ROWS, 2 * ROWS)
    row_noise = jax.random.randint(jax.random.fold_in(key, 17), (NLAT,), -2 * ROWS, 2 * ROWS + 1)
    offsets = jnp.clip(row_drift + row_noise, -REACH * ROWS + 1, REACH * ROWS - 2)
    spread = jax.random.randint(jax.random.fold_in(key, 29), (NLAT,), 0, 1 << 20)
    north_offset = -(1 + spread % (REACH * ROWS - 1))
    south_offset = 1 + spread % (REACH * ROWS - 2)
    position = row_ids % ROWS
    offsets = jnp.where(position == 0, north_offset, offsets)
    offsets = jnp.where(position == ROWS - 1, south_offset, offsets)
    return jnp.clip(row_ids + offsets, 1, NLAT - 3).astype(jnp.int32)


def plant(array, rng, low, largest):
    spot = [jax.random.randint(jax.random.fold_in(rng, axis), (), 0, length) for axis, length in enumerate(array.shape)]
    widest = array.shape.index(max(array.shape))
    next_to = spot[:widest] + [(spot[widest] + 1) % array.shape[widest]] + spot[widest + 1:]
    return array.at[tuple(spot)].set(low).at[tuple(next_to)].set(largest)


def level_of(stream_key, shape, pieces, smallest, high):
    def one(axis_at, blocks):
        heights = jax.random.uniform(jax.random.fold_in(jax.random.fold_in(stream_key, 6), axis_at), (blocks,), jnp.float32, smallest / len(pieces), high / len(pieces))
        return jnp.repeat(jnp.exp(heights), shape[axis_at] // blocks).reshape((-1,) + (1,) * (len(shape) - axis_at - 1))

    gain = one(*pieces[0])
    for cut in pieces[1:]:
        gain = gain * one(*cut)
    return gain


def setup_inputs(seed: int = 0) -> dict:
    key_of = jax.random.split(jax.random.key(seed), 7)
    return {
        "fields": draw_fields(jax.random.fold_in(key_of[6], 71), 0),
        "lat_fraction": jnp.clip(1.0 * jax.random.uniform(key_of[1], (NLAT,), jnp.float32) ** level_of(key_of[1], (NLAT,), ((0, 128),), -0.2, 0.2), 0.0, 1.0),
        "lon_fraction": jnp.clip(1.0 * jax.random.uniform(key_of[2], (NLAT,), jnp.float32) ** level_of(key_of[2], (NLAT,), ((0, 128),), -0.2, 0.2), 0.0, 1.0),
        "lon_shift": plant(jax.random.randint(key_of[3], (NLAT,), 0, LON), jax.random.fold_in(key_of[3], 1), 0, LON - 1).astype(jnp.int32),
        "departure_row": draw_departure_row(jax.random.fold_in(key_of[6], 71), 0),
        "extents": plant(jax.random.randint(key_of[5], (BANDS, 2), 1, REACH + 1), jax.random.fold_in(key_of[5], 1), 1, REACH).astype(jnp.int32),
    }


def cubic_weights(fraction):
    return jnp.stack([-fraction * (fraction - 1.0) * (fraction - 2.0) / 6.0,
                      (fraction + 1.0) * (fraction - 1.0) * (fraction - 2.0) / 2.0,
                      -(fraction + 1.0) * fraction * (fraction - 2.0) / 2.0,
                      (fraction + 1.0) * fraction * (fraction - 1.0) / 6.0])


def along_lon(column, lon_w, shift_value):
    lon_count = column.shape[-1]
    doubled = jnp.concatenate([column, column], axis=-1)
    result = jnp.zeros_like(column)
    for offset in range(4):
        first = ((shift_value + offset - 1) % lon_count).astype(jnp.int32)
        result = result + lon_w[offset] * lax.dynamic_slice_in_dim(doubled, first, lon_count, 2)
    return result


def reference(fields, lat_fraction, lon_fraction, lon_shift, departure_row, extents):
    row_ids = jnp.arange(NLAT, dtype=jnp.int32)
    band_ids = row_ids // ROWS
    low_bound = band_ids * ROWS - extents[band_ids, 0] * ROWS + 1
    high_bound = band_ids * ROWS + ROWS - 3 + extents[band_ids, 1] * ROWS
    departure = jnp.clip(jnp.clip(departure_row, low_bound, high_bound), 1, NLAT - 3).astype(jnp.int32)

    def one_row(inputs):
        dep_value, lat_t, lon_t, shift_value = inputs
        row_block = lax.dynamic_slice_in_dim(fields, (dep_value - 1).astype(jnp.int32), 4, 0)
        lat_w = cubic_weights(lat_t)
        column = lat_w[0] * row_block[0] + lat_w[1] * row_block[1] + lat_w[2] * row_block[2] + lat_w[3] * row_block[3]
        return along_lon(column, cubic_weights(lon_t), shift_value)

    moved = lax.map(one_row, (departure, lat_fraction, lon_fraction, lon_shift))
    area = jnp.cos(math.pi * (row_ids.astype(jnp.float32) + 0.5) / NLAT - math.pi / 2.0)
    mass_before = jnp.sum(area[:, None, None, None] * fields, axis=(0, 2, 3))
    mass_after = jnp.sum(area[:, None, None, None] * moved, axis=(0, 2, 3))
    return moved * (mass_before / mass_after)[None, :, None, None]
```

```python
import functools
import math

import jax
import jax.numpy as jnp
from jax import lax
from jax.experimental import pallas as pl
from jax.experimental.pallas import tpu as pltpu
from jax.sharding import PartitionSpec as P

MESH = pl.DeviceIdType.MESH
NY, NZ, NX = 4, 8, 4
LANES = 128
SPLITS = 2
ROWS_PER_STEP = 2


def cubic_weights(fraction):
    return [
        -fraction * (fraction - 1.0) * (fraction - 2.0) / 6.0,
        (fraction + 1.0) * (fraction - 1.0) * (fraction - 2.0) / 2.0,
        -(fraction + 1.0) * fraction * (fraction - 2.0) / 2.0,
        (fraction + 1.0) * fraction * (fraction - 1.0) / 6.0,
    ]


def advect_kernel(rows, nfields, lon, chunks, itab_ref, ftab_ref, fields_ref, out_ref, ratio_ref, *scratch):
    count = len(chunks)
    scratch = list(scratch)
    rings = [scratch.pop(0) for _ in range(count)]
    send_up = [scratch.pop(0) for _ in range(count)]
    send_down = [scratch.pop(0) for _ in range(count)]
    recv_up = [scratch.pop(0) for _ in range(count)]
    recv_down = [scratch.pop(0) for _ in range(count)]
    (out_buf, sums, itab_far, ftab_far, itab, ftab, mass,
     load_sem, own_send, own_recv, fwd_send, fwd_recv, z_send, z_recv,
     tab_send, tab_recv, tab_local, sum_send, sum_recv, mass_send, mass_recv, out_sem) = scratch

    band = lax.axis_index("lat")
    core = lax.axis_index("lev")
    bands = NX * NZ * NY
    y = lax.rem(band, NY)
    z = lax.rem(lax.div(band, NY), NZ)
    x = lax.div(band, NY * NZ)
    base = band - y
    ring_rows = NY * rows
    first_ring_row = lax.div(band, NY) * ring_rows

    def in_ring(step):
        return base + lax.rem(y + step, NY)

    y_up, y_far, y_down = [lax.rem(y + s, NY) for s in (1, 2, 3)]
    y_mates = [(in_ring(s), core) for s in (1, 2, 3)]
    z_mates = [(x * (NY * NZ) + lax.rem(z + s, NZ) * NY + y, core) for s in range(1, NZ)]
    x_mates = [(lax.rem(x + s, NX) * (NY * NZ) + z * NY + y, core) for s in range(1, NX)]
    c_mates = [(band, 1 - core)]
    up = (lax.rem(band + NY, bands), core)
    down = (lax.rem(band + bands - NY, bands), core)
    partners = y_mates + z_mates + x_mates + c_mates + [up, down]

    loads = [
        pltpu.make_async_copy(
            fields_ref.at[:, f, :, pl.ds(lane, width)], rings[c].at[pl.ds(y * rows, rows)], load_sem.at[c]
        )
        for c, (f, lane, width) in enumerate(chunks)
    ]
    for load in loads:
        load.start()
    tab_own = [
        pltpu.make_async_copy(itab_ref, itab.at[0], tab_local.at[0]),
        pltpu.make_async_copy(ftab_ref, ftab.at[0], tab_local.at[1]),
    ]
    for copy in tab_own:
        copy.start()

    barrier = pltpu.get_barrier_semaphore()
    for partner in partners:
        pl.semaphore_signal(barrier, inc=1, device_id=partner, device_id_type=MESH)
    pl.semaphore_wait(barrier, len(partners))

    def remote(src, dst, send_sem, recv_sem, target):
        return pltpu.make_async_remote_copy(
            src_ref=src, dst_ref=dst, send_sem=send_sem, recv_sem=recv_sem, device_id=target, device_id_type=MESH
        )

    tables = [
        remote(itab_ref, itab_far.at[1], tab_send.at[0], tab_recv.at[0], up),
        remote(itab_ref, itab_far.at[0], tab_send.at[1], tab_recv.at[1], down),
        remote(ftab_ref, ftab_far.at[1], tab_send.at[2], tab_recv.at[2], up),
        remote(ftab_ref, ftab_far.at[0], tab_send.at[3], tab_recv.at[3], down),
    ]
    for copy in tables:
        copy.start()

    half = rows // 2
    owns, forwards, zsends = [], [], []
    for c in range(count):
        mine = rings[c].at[pl.ds(y * rows, rows)]
        owns.append([
            remote(mine, mine, own_send.at[c, 0], own_recv.at[c, 0], y_mates[0]),
            remote(mine, mine, own_send.at[c, 1], own_recv.at[c, 1], y_mates[2]),
        ])
        from_down = rings[c].at[pl.ds(y_down * rows + half, rows - half)]
        from_up = rings[c].at[pl.ds(y_up * rows, half)]
        forwards.append([
            remote(from_down, from_down, fwd_send.at[c, 0], fwd_recv.at[c, 0], y_mates[0]),
            remote(from_up, from_up, fwd_send.at[c, 1], fwd_recv.at[c, 1], y_mates[2]),
        ])
        zsends.append([
            remote(send_up[c], recv_up[c], z_send.at[c, 0], z_recv.at[c, 0], up),
            remote(send_down[c], recv_down[c], z_send.at[c, 1], z_recv.at[c, 1], down),
        ])

    for c in range(2):
        loads[c].wait()
        for copy in owns[c]:
            copy.start()
    for c in range(2, count):
        loads[c].wait()

    def row_sums(r, carry):
        pieces = []
        for f in range(nfields):
            total = None
            for c, (field, lane, width) in enumerate(chunks):
                if field != f:
                    continue
                block = rings[c][y * rows + r]
                for t in range(width // LANES):
                    tile = block[:, t * LANES:(t + 1) * LANES]
                    total = tile if total is None else total + tile
            pieces.append(jnp.sum(total, axis=0, keepdims=True))
        pieces.append(jnp.zeros((8 - nfields, LANES), jnp.float32))
        sums[y * rows + r] = jnp.concatenate(pieces, axis=0)
        return carry

    lax.fori_loop(0, rows, row_sums, 0)

    for copy in tab_own:
        copy.wait()
    for copy in tables:
        copy.wait_recv()
    tab_in = [
        pltpu.make_async_copy(itab_far.at[0], itab.at[1], tab_local.at[2]),
        pltpu.make_async_copy(itab_far.at[1], itab.at[2], tab_local.at[3]),
        pltpu.make_async_copy(ftab_far.at[0], ftab.at[1], tab_local.at[4]),
        pltpu.make_async_copy(ftab_far.at[1], ftab.at[2], tab_local.at[5]),
    ]
    for copy in tab_in:
        copy.start()
    my_sums = sums.at[pl.ds(y * rows, rows)]
    sum_copies = [remote(my_sums, my_sums, sum_send.at[s], sum_recv.at[s], y_mates[s]) for s in range(NY - 1)]
    for copy in sum_copies:
        copy.start()
    for copy in tab_in:
        copy.wait()

    def taps(t, r):
        first = itab[t, 0, r] - first_ring_row
        out = []
        for a in range(4):
            spot = first + a
            inside = jnp.logical_and(spot >= 0, spot < ring_rows)
            out.append((jnp.clip(spot, 0, ring_rows - 1), jnp.where(inside, ftab[t, a, r], 0.0)))
        return out

    def partial_rows(t, c, dst):
        def one(r, carry):
            acc = None
            for spot, weight in taps(t, r):
                term = weight * rings[c][spot]
                acc = term if acc is None else acc + term
            dst[r] = acc
            return carry

        lax.fori_loop(0, rows, one, 0)

    phases = [x_mates, c_mates, z_mates, y_mates]
    offsets = [0]
    for mates in phases:
        offsets.append(offsets[-1] + len(mates))
    mass_copies = []
    for k, mates in enumerate(phases):
        mass_copies.append([
            remote(mass.at[k], mass.at[len(phases) + 1 + offsets[k] + i], mass_send.at[offsets[k] + i],
                   mass_recv.at[offsets[k] + i], mate)
            for i, mate in enumerate(mates)
        ])

    def mass_step(step):
        if step == 0:
            for copy in sum_copies:
                copy.wait_recv()

            def one(r, carry):
                before, after = carry
                before = before + ftab[0, 9, r] * sums[y * rows + r]
                for t in range(3):
                    moved = None
                    for spot, weight in taps(t, r):
                        term = weight * sums[spot]
                        moved = term if moved is None else moved + term
                    after = after + ftab[t, 4, r] * moved
                return before, after

            zero = jnp.zeros((8, LANES), jnp.float32)
            before, after = lax.fori_loop(0, rows, one, (zero, zero))
        elif step <= len(phases):
            k = step - 1
            before, after = mass[k, 0:8], mass[k, 8:16]
            for i, copy in enumerate(mass_copies[k]):
                copy.wait_recv()
                slot = len(phases) + 1 + offsets[k] + i
                before = before + mass[slot, 0:8]
                after = after + mass[slot, 8:16]
        else:
            return
        if step < len(phases):
            mass[step, 0:8] = before
            mass[step, 8:16] = after
            for copy in mass_copies[step]:
                copy.start()
        else:
            before = jnp.sum(before, axis=1, keepdims=True)
            after = jnp.sum(after, axis=1, keepdims=True)
            ratio_ref[...] = jnp.broadcast_to(before / after, (8, LANES))

    outs = [pltpu.make_async_copy(out_buf.at[f], out_ref.at[:, f], out_sem.at[f]) for f in range(nfields)]

    def finish(f):
        mine = [c for c, chunk in enumerate(chunks) if chunk[0] == f]
        for c in mine:
            for copy in zsends[c]:
                copy.wait_recv()

        def one(r, carry):
            spots = taps(0, r)
            for c in mine:
                _, lane, width = chunks[c]
                acc = recv_up[c][r] + recv_down[c][r]
                for spot, weight in spots:
                    acc = acc + weight * rings[c][spot]
                out_buf[f, r, :, lane:lane + width] = acc
            return carry

        lax.fori_loop(0, rows, one, 0)
        outs[f].start()

    finished = 0
    for c in range(count):
        for copy in owns[c]:
            copy.wait_recv()
        for copy in forwards[c]:
            copy.start()
        if c + 2 < count:
            for copy in owns[c + 2]:
                copy.start()
        for copy in forwards[c]:
            copy.wait_recv()
        partial_rows(1, c, send_up[c])
        partial_rows(2, c, send_down[c])
        for copy in zsends[c]:
            copy.start()
        mass_step(c)
        if c >= len(phases):
            while finished < nfields and chunks[c][0] > finished:
                finish(finished)
                finished += 1
    for step in range(count, len(phases) + 1):
        mass_step(step)
    while finished < nfields:
        finish(finished)
        finished += 1

    for c in range(count):
        for copy in owns[c] + forwards[c] + zsends[c]:
            copy.wait_send()
    for copy in tables + sum_copies:
        copy.wait_send()
    for group in mass_copies:
        for copy in group:
            copy.wait_send()
    for copy in outs:
        copy.wait()


def turn_kernel(nfields, lon, itab, ftab, ratio_ref, column_ref, out_ref, doubled):
    lane_id = lax.broadcasted_iota(jnp.int32, (8, LANES), 1)
    tiles = lon // LANES
    size = lon + 2 * LANES
    for i in range(ROWS_PER_STEP):
        r = pl.program_id(0) * ROWS_PER_STEP + i
        begin = itab[1, r]
        whole = pl.multiple_of(lax.shift_right_logical(begin, 7) * LANES, LANES)
        rest = jnp.bitwise_and(begin, LANES - 1)
        turn = jnp.bitwise_and(LANES - rest, LANES - 1)
        keep = lane_id < (LANES - rest)
        for f in range(nfields):
            column = column_ref[i, f]
            doubled[:, 0:lon] = column
            doubled[:, lon:2 * lon] = column
            doubled[:, 2 * lon:2 * lon + 2 * LANES] = column[:, :2 * LANES]
            window = doubled[:, pl.ds(whole, size)]
            mixed = ftab[5, r] * window
            for k in range(1, 4):
                mixed = mixed + ftab[5 + k, r] * pltpu.roll(window, size - k, 1)
            mixed = mixed * jnp.broadcast_to(ratio_ref[f:f + 1, 0:1], (8, size))
            turned = [pltpu.roll(mixed[:, t * LANES:(t + 1) * LANES], turn, 1) for t in range(tiles + 1)]
            for t in range(tiles):
                out_ref[i, f, :, t * LANES:(t + 1) * LANES] = jnp.where(keep, turned[t], turned[t + 1])


def per_device(fields, lat_fraction, lon_fraction, lon_shift, departure_row, extents):
    rows, nfields, levels, lon = fields.shape
    bands = NX * NZ * NY
    total_rows = bands * rows
    band = lax.axis_index("lat")
    first_row = band * rows
    low = first_row - extents[0, 0] * rows + 1
    high = first_row + rows - 3 + extents[0, 1] * rows
    start = jnp.clip(jnp.clip(departure_row, low, high), 1, total_rows - 3) - 1
    begin = lax.rem(lon_shift + (lon - 1), lon)
    itab = jnp.pad(jnp.stack([start, begin]), ((0, 6), (0, LANES - rows)))
    lat_w = cubic_weights(lat_fraction)
    lon_w = cubic_weights(lon_fraction)
    row_ids = first_row + jnp.arange(rows, dtype=jnp.int32)
    area = jnp.cos(math.pi * (row_ids.astype(jnp.float32) + 0.5) / total_rows - math.pi / 2.0)
    lon_total = lon_w[0] + lon_w[1] + lon_w[2] + lon_w[3]
    ftab = jnp.pad(jnp.stack(lat_w + [area * lon_total] + lon_w + [area]), ((0, 6), (0, LANES - rows)))

    width = lon // SPLITS
    chunks = [(f, s * width, width) for f in range(nfields) for s in range(SPLITS)]
    count = len(chunks)
    dma = pltpu.SemaphoreType.DMA
    mates = (NX - 1) + 1 + (NZ - 1) + (NY - 1)
    scratch = [pltpu.VMEM((NY * rows, levels, w), jnp.float32) for _, _, w in chunks]
    for _ in range(4):
        scratch += [pltpu.VMEM((rows, levels, w), jnp.float32) for _, _, w in chunks]
    scratch += [
        pltpu.VMEM((nfields, rows, levels, lon), jnp.float32),
        pltpu.VMEM((NY * rows, 8, LANES), jnp.float32),
        pltpu.VMEM((2, 8, LANES), jnp.int32),
        pltpu.VMEM((2, 16, LANES), jnp.float32),
        pltpu.SMEM((3, 8, LANES), jnp.int32),
        pltpu.SMEM((3, 16, LANES), jnp.float32),
        pltpu.VMEM((5 + mates, 16, LANES), jnp.float32),
        dma((count,)), dma((count, 2)), dma((count, 2)), dma((count, 2)), dma((count, 2)), dma((count, 2)), dma((count, 2)),
        dma((4,)), dma((4,)), dma((6,)), dma((NY - 1,)), dma((NY - 1,)), dma((mates,)), dma((mates,)), dma((nfields,)),
    ]
    column, ratio = pl.pallas_call(
        functools.partial(advect_kernel, rows, nfields, lon, chunks),
        out_shape=(
            jax.ShapeDtypeStruct(fields.shape, fields.dtype),
            jax.ShapeDtypeStruct((8, LANES), jnp.float32),
        ),
        in_specs=[
            pl.BlockSpec(memory_space=pltpu.VMEM),
            pl.BlockSpec(memory_space=pltpu.VMEM),
            pl.BlockSpec(memory_space=pl.ANY),
        ],
        out_specs=(pl.BlockSpec(memory_space=pl.ANY), pl.BlockSpec(memory_space=pltpu.VMEM)),
        scratch_shapes=scratch,
        compiler_params=pltpu.CompilerParams(collective_id=0, has_side_effects=True),
    )(itab, ftab, fields)
    block = pl.BlockSpec((ROWS_PER_STEP, nfields, levels, lon), lambda i: (i, 0, 0, 0))
    return pl.pallas_call(
        functools.partial(turn_kernel, nfields, lon),
        grid=(rows // ROWS_PER_STEP,),
        out_shape=jax.ShapeDtypeStruct(fields.shape, fields.dtype),
        in_specs=[
            pl.BlockSpec(memory_space=pltpu.SMEM),
            pl.BlockSpec(memory_space=pltpu.SMEM),
            pl.BlockSpec(memory_space=pltpu.VMEM),
            block,
        ],
        out_specs=block,
        scratch_shapes=[pltpu.VMEM((levels, 2 * lon + 2 * LANES), jnp.float32)],
    )(itab, ftab, ratio, column)


def solution(mesh):
    placed = (P("lat", None, "lev", None), P("lat"), P("lat"), P("lat"), P("lat"), P("lat", None))
    return jax.shard_map(
        per_device,
        mesh=mesh,
        in_specs=placed,
        out_specs=P("lat", None, "lev", None),
        check_vma=False,
    )
```

```python
import functools
import math

import jax
import jax.numpy as jnp
from jax import lax
from jax.experimental import pallas as pl
from jax.experimental.pallas import tpu as pltpu
from jax.sharding import PartitionSpec as P

MESH = pl.DeviceIdType.MESH
NY, NZ, NX = 4, 8, 4
LANES = 128
ROWS_PER_STEP = 2
CHUNKS = [('ring', 1, 1, 1, 2), ('pair', 2, 1, 1, 2), ('pair', 0, 1, 1, 2), ('column', 0, 0, 1, 2), ('column', 2, 0, 1, 2), ('column', 1, 0, 1, 2)]
ORDER = [0, 3, 2, 5, 3, 0, 4, 5, 2, 1, 3, 4, 5, 0, 2, 1, 4, 3, 2, 0, 1, 4, 5, 1]
MASS_AT = [6, 9, 12, 15, 18]


def cubic_weights(fraction):
    return [
        -fraction * (fraction - 1.0) * (fraction - 2.0) / 6.0,
        (fraction + 1.0) * (fraction - 1.0) * (fraction - 2.0) / 2.0,
        -(fraction + 1.0) * fraction * (fraction - 2.0) / 2.0,
        (fraction + 1.0) * fraction * (fraction - 1.0) / 6.0,
    ]


def buffers_of(scheme, rows, levels, width):
    half = rows // 2
    counts = {
        "ring": [NY * rows] + [rows] * 4,
        "column": [3 * rows] + [rows] * 3 + [half, rows - half] + [rows] * 2,
        "pair": [2 * rows] + [rows] * 8,
    }[scheme]
    return [pltpu.VMEM((n, levels, width), jnp.float32) for n in counts]


COPIES = {"ring": 6, "column": 6, "pair": 5}


def advect_kernel(rows, nfields, lon, chunks, *refs):
    refs = list(refs)
    lat_ref, lon_ref, departure_ref, extents_ref, fields_ref, out_ref, ratio_ref = refs[:7]
    scratch = refs[7:]
    count = len(chunks)
    bufs = []
    for chunk in chunks:
        n = len(buffers_of(chunk[0], rows, 8, LANES))
        bufs.append(scratch[:n])
        scratch = scratch[n:]
    (out_buf, sums, itab_all, ftab_all, itab, ftab, mass,
     load_sem, bulk_send, bulk_recv, tab_send, tab_recv, tab_local,
     sum_send, sum_recv, mass_send, mass_recv, out_sem) = scratch

    band = lax.axis_index("lat")
    core = lax.axis_index("lev")
    bands = NX * NZ * NY
    y = lax.rem(band, NY)
    z = lax.rem(lax.div(band, NY), NZ)
    x = lax.div(band, NY * NZ)
    base = band - y
    odd = lax.rem(y, 2)
    south = lax.div(y, 2)

    y_up, y_down = lax.rem(y + 1, NY), lax.rem(y + 3, NY)
    y_mates = [(base + lax.rem(y + s, NY), core) for s in (1, 2, 3)]
    z_mates = [(x * (NY * NZ) + lax.rem(z + s, NZ) * NY + y, core) for s in range(1, NZ)]
    x_mates = [(lax.rem(x + s, NX) * (NY * NZ) + z * NY + y, core) for s in range(1, NX)]
    c_mates = [(band, 1 - core)]
    up = (lax.rem(band + NY, bands), core)
    down = (lax.rem(band + bands - NY, bands), core)
    pair = (band + 1 - 2 * odd, core)
    cross = (base + 3 - y, core)
    toward = (lax.rem(band + bands - NY + 2 * NY * south, bands), core)
    diagonal = (lax.rem(base + 3 - y + bands - NY + 2 * NY * south, bands), core)
    partners = y_mates + z_mates + x_mates + c_mates + [up, down, diagonal]

    own_at = {"ring": y * rows, "column": rows, "pair": odd * rows}
    loads = [
        pltpu.make_async_copy(
            fields_ref.at[:, f, :, pl.ds(lane, width)],
            bufs[c][0].at[pl.ds(own_at[scheme], rows)],
            load_sem.at[c],
        )
        for c, (scheme, f, lane, width) in enumerate(chunks)
    ]
    loaded_first = []
    for c in ORDER + list(range(count)):
        if c not in loaded_first:
            loaded_first.append(c)
    for c in loaded_first:
        loads[c].start()

    barrier = pltpu.get_barrier_semaphore()
    for partner in partners:
        pl.semaphore_signal(barrier, inc=1, device_id=partner, device_id_type=MESH)

    first_row = band * rows
    low = first_row - extents_ref[0:1, 0:1] * rows + 1
    high = first_row + rows - 3 + extents_ref[0:1, 1:2] * rows
    start = jnp.minimum(jnp.maximum(departure_ref[...], low), high)
    start = jnp.minimum(jnp.maximum(start, 1), bands * rows - 3) - 1
    lat_w = cubic_weights(lat_ref[...])
    lon_w = cubic_weights(lon_ref[...])
    row_ids = first_row + lax.broadcasted_iota(jnp.int32, (1, rows), 1)
    area = jnp.cos(math.pi * (row_ids.astype(jnp.float32) + 0.5) / (bands * rows) - math.pi / 2.0)
    lon_total = lon_w[0] + lon_w[1] + lon_w[2] + lon_w[3]
    itab_all[0] = jnp.zeros((8, LANES), jnp.int32)
    ftab_all[0] = jnp.zeros((16, LANES), jnp.float32)
    itab_all[0, 0:1, 0:rows] = start
    for k, values in enumerate(lat_w + [area * lon_total] + lon_w + [area]):
        ftab_all[0, k:k + 1, 0:rows] = values

    for load in loads:
        load.wait()

    def row_sums(r, carry):
        pieces = []
        for f in range(nfields):
            total = None
            for c, (scheme, field, lane, width) in enumerate(chunks):
                if field != f:
                    continue
                block = bufs[c][0][own_at[scheme] + r]
                for t in range(width // LANES):
                    tile = block[:, t * LANES:(t + 1) * LANES]
                    total = tile if total is None else total + tile
            pieces.append(jnp.sum(total, axis=0, keepdims=True))
        pieces.append(jnp.zeros((8 - nfields, LANES), jnp.float32))
        sums[y * rows + r] = jnp.concatenate(pieces, axis=0)
        return carry

    lax.fori_loop(0, rows, row_sums, 0)
    pl.semaphore_wait(barrier, len(partners))

    def remote(src, dst, send_sem, recv_sem, target):
        return pltpu.make_async_remote_copy(
            src_ref=src, dst_ref=dst, send_sem=send_sem, recv_sem=recv_sem, device_id=target, device_id_type=MESH
        )

    table_routes = [(2, up), (1, down), (5, y_mates[0]), (4, y_mates[1]), (3, y_mates[2]), (6, diagonal)]
    tables = []
    for i, (slot, target) in enumerate(table_routes):
        for j, ref in enumerate((itab_all, ftab_all)):
            tables.append(remote(ref.at[0], ref.at[slot], tab_send.at[2 * i + j], tab_recv.at[2 * i + j], target))
    for copy in tables:
        copy.start()
    my_sums = sums.at[pl.ds(y * rows, rows)]
    sum_copies = [remote(my_sums, my_sums, sum_send.at[s], sum_recv.at[s], y_mates[s]) for s in range(NY - 1)]

    def ring_spot(row):
        spot = row - base * rows
        return jnp.clip(spot, 0, NY * rows - 1), jnp.logical_and(spot >= 0, spot < NY * rows)

    def pair_spot(row):
        spot = row - (band - odd) * rows
        return jnp.clip(spot, 0, 2 * rows - 1), jnp.logical_and(spot >= 0, spot < 2 * rows)

    def column_spot(row):
        away = row - (band - NY) * rows
        block = (away >= NY * rows).astype(jnp.int32) + (away >= 2 * NY * rows).astype(jnp.int32)
        within = away - block * (NY * rows)
        return block * rows + jnp.clip(within, 0, rows - 1), jnp.logical_and(within >= 0, within < rows)

    def taps(spot_of, t, r):
        first = itab[t, 0, r]
        out = []
        for a in range(4):
            spot, inside = spot_of(first + a)
            out.append((spot, jnp.where(inside, ftab[t, a, r], 0.0)))
        return out

    def weighted(ref, spots):
        acc = None
        for spot, weight in spots:
            term = weight * ref[spot]
            acc = term if acc is None else acc + term
        return acc

    def partial_rows(spot_of, src, jobs):
        def one(r, carry):
            for t, dst, extra in jobs:
                acc = weighted(src, taps(spot_of, t, r))
                dst[r] = acc if extra is None else acc + extra[r]
            return carry

        lax.fori_loop(0, rows, one, 0)

    def add_rows(n, dst, dst_at, extra):
        def one(r, carry):
            dst[dst_at + r] = dst[dst_at + r] + extra[r]
            return carry

        lax.fori_loop(0, n, one, 0)

    ready = []

    def need_tables():
        if ready:
            return
        ready.append(True)
        for copy in tables:
            copy.wait_recv()
        moves = [
            pltpu.make_async_copy(itab_all, itab, tab_local.at[0]),
            pltpu.make_async_copy(ftab_all, ftab, tab_local.at[1]),
        ]
        for copy in moves:
            copy.start()
        for copy in moves:
            copy.wait()

    half = rows // 2
    finals = [None] * count

    def stages_of(c):
        scheme = chunks[c][0]
        b = bufs[c]
        send = [bulk_send.at[c, k] for k in range(COPIES[scheme])]
        recv = [bulk_recv.at[c, k] for k in range(COPIES[scheme])]

        def link(k, src, dst, target):
            return remote(src, dst, send[k], recv[k], target)

        if scheme == "ring":
            ring, send_up, send_down, recv_up, recv_down = b
            mine = ring.at[pl.ds(y * rows, rows)]
            from_down = ring.at[pl.ds(y_down * rows + half, rows - half)]
            from_up = ring.at[pl.ds(y_up * rows, half)]
            copies = [
                link(0, mine, mine, y_mates[0]), link(1, mine, mine, y_mates[2]),
                link(2, from_down, from_down, y_mates[0]), link(3, from_up, from_up, y_mates[2]),
                link(4, send_up, recv_up, up), link(5, send_down, recv_down, down),
            ]

            def stage0():
                copies[0].start()
                copies[1].start()

            def stage1():
                copies[0].wait_recv()
                copies[1].wait_recv()
                copies[2].start()
                copies[3].start()

            def stage2():
                copies[2].wait_recv()
                copies[3].wait_recv()
                need_tables()
                partial_rows(ring_spot, ring, [(1, send_up, None), (2, send_down, None)])
                copies[4].start()
                copies[5].start()

            def stage3():
                copies[4].wait_recv()
                copies[5].wait_recv()
                finals[c] = (ring_spot, ring, [recv_up, recv_down])

        elif scheme == "column":
            column, to_up, to_down, to_far, far_a, far_b, got_a, got_b = b
            mine = column.at[pl.ds(rows, rows)]
            copies = [
                link(0, mine, column.at[pl.ds(0, rows)], up), link(1, mine, column.at[pl.ds(2 * rows, rows)], down),
                link(2, to_far.at[pl.ds(0, half)], far_a, y_mates[0]),
                link(3, to_far.at[pl.ds(half, rows - half)], far_b, y_mates[2]),
                link(4, to_up, got_a, y_mates[0]), link(5, to_down, got_b, y_mates[2]),
            ]

            def stage0():
                copies[0].start()
                copies[1].start()

            def stage1():
                copies[0].wait_recv()
                copies[1].wait_recv()
                need_tables()
                partial_rows(column_spot, column, [(4, to_far, None)])
                copies[2].start()
                copies[3].start()
                partial_rows(column_spot, column, [(3, to_up, None), (5, to_down, None)])

            def stage2():
                copies[2].wait_recv()
                add_rows(half, to_up, 0, far_a)
                copies[4].start()
                copies[3].wait_recv()
                add_rows(rows - half, to_down, half, far_b)
                copies[5].start()

            def stage3():
                copies[4].wait_recv()
                copies[5].wait_recv()
                finals[c] = (column_spot, column, [got_a, got_b])

        else:
            both, to_up, to_down, to_diag, to_cross, from_down, from_up, passed, from_cross = b
            mine = both.at[pl.ds(odd * rows, rows)]
            copies = [
                link(0, mine, mine, pair), link(1, to_up, from_down, up), link(2, to_down, from_up, down),
                link(3, to_diag, passed, toward), link(4, to_cross, from_cross, cross),
            ]

            def stage0():
                copies[0].start()

            def stage1():
                copies[0].wait_recv()
                need_tables()
                partial_rows(pair_spot, both, [(6, to_diag, None)])
                copies[3].start()
                partial_rows(pair_spot, both, [(1, to_up, None), (2, to_down, None)])
                copies[1].start()
                copies[2].start()

            def stage2():
                copies[3].wait_recv()
                partial_rows(pair_spot, both, [(5 - 2 * odd, to_cross, passed)])
                copies[4].start()

            def stage3():
                copies[1].wait_recv()
                copies[2].wait_recv()
                copies[4].wait_recv()
                finals[c] = (pair_spot, both, [from_down, from_up, from_cross])

        return copies, [stage0, stage1, stage2, stage3]

    phases = [x_mates, c_mates, z_mates, y_mates]
    offsets = [0]
    for mates in phases:
        offsets.append(offsets[-1] + len(mates))
    mass_copies = []
    for k, mates in enumerate(phases):
        mass_copies.append([
            remote(mass.at[k], mass.at[len(phases) + offsets[k] + i], mass_send.at[offsets[k] + i],
                   mass_recv.at[offsets[k] + i], mate)
            for i, mate in enumerate(mates)
        ])

    def mass_step(step):
        if step == 0:
            need_tables()
            for copy in sum_copies:
                copy.wait_recv()

            def one(r, carry):
                before, after = carry
                before = before + ftab[0, 9, r] * sums[y * rows + r]
                for t in range(3):
                    after = after + ftab[t, 4, r] * weighted(sums, taps(ring_spot, t, r))
                return before, after

            zero = jnp.zeros((8, LANES), jnp.float32)
            before, after = lax.fori_loop(0, rows, one, (zero, zero))
        else:
            k = step - 1
            before, after = mass[k, 0:8], mass[k, 8:16]
            for i, copy in enumerate(mass_copies[k]):
                copy.wait_recv()
                slot = len(phases) + offsets[k] + i
                before = before + mass[slot, 0:8]
                after = after + mass[slot, 8:16]
        if step < len(phases):
            mass[step, 0:8] = before
            mass[step, 8:16] = after
            for copy in mass_copies[step]:
                copy.start()
        else:
            before = jnp.sum(before, axis=1, keepdims=True)
            after = jnp.sum(after, axis=1, keepdims=True)
            ratio_ref[...] = jnp.broadcast_to(before / after, (8, LANES))

    outs = [pltpu.make_async_copy(out_buf.at[f], out_ref.at[:, f], out_sem.at[f]) for f in range(nfields)]

    def finish(c):
        _, f, lane, width = chunks[c]
        spot_of, src, extras = finals[c]

        def one(r, carry):
            acc = weighted(src, taps(spot_of, 0, r))
            for extra in extras:
                acc = acc + extra[r]
            out_buf[f, r, :, lane:lane + width] = acc
            return carry

        lax.fori_loop(0, rows, one, 0)

    def filter_rows(f):
        def one(r, carry):
            column = out_buf[f, r]
            mixed = ftab[0, 5, r] * column
            for k in range(1, 4):
                mixed = mixed + ftab[0, 5 + k, r] * pltpu.roll(column, lon - k, 1)
            out_buf[f, r] = mixed
            return carry

        lax.fori_loop(0, rows, one, 0)
        outs[f].start()

    every = [stages_of(c) for c in range(count)]
    place = [0] * count
    left = [sum(1 for chunk in chunks if chunk[1] == f) for f in range(nfields)]
    mass_done = 0
    for i, c in enumerate(ORDER):
        every[c][1][place[c]]()
        place[c] += 1
        if i == 1:
            for copy in sum_copies:
                copy.start()
        if place[c] == 4:
            finish(c)
            f = chunks[c][1]
            left[f] -= 1
            if left[f] == 0:
                filter_rows(f)
        while mass_done < len(MASS_AT) and MASS_AT[mass_done] == i:
            mass_step(mass_done)
            mass_done += 1

    for copies, _ in every:
        for copy in copies:
            copy.wait_send()
    for copy in tables + sum_copies:
        copy.wait_send()
    for group in mass_copies:
        for copy in group:
            copy.wait_send()
    for copy in outs:
        copy.wait()


def turn_kernel(nfields, lon, shift_ref, ratio_ref, column_ref, out_ref):
    lane_id = lax.broadcasted_iota(jnp.int32, (8, LANES), 1)
    tiles = lon // LANES
    for i in range(ROWS_PER_STEP):
        r = pl.program_id(0) * ROWS_PER_STEP + i
        begin = shift_ref[r] - 1
        begin = jnp.where(begin < 0, begin + lon, begin)
        whole = lax.shift_right_logical(begin, 7)
        rest = jnp.bitwise_and(begin, LANES - 1)
        turn = jnp.bitwise_and(LANES - rest, LANES - 1)
        keep = lane_id < (LANES - rest)
        spots = []
        for t in range(tiles + 1):
            spot = whole + t
            spot = jnp.where(spot >= tiles, spot - tiles, spot)
            spots.append(pl.multiple_of(spot * LANES, LANES))
        for f in range(nfields):
            ratio = jnp.broadcast_to(ratio_ref[f:f + 1, :], (8, LANES))
            turned = [pltpu.roll(column_ref[i, f, :, pl.ds(spot, LANES)], turn, 1) for spot in spots]
            for t in range(tiles):
                out_ref[i, f, :, t * LANES:(t + 1) * LANES] = jnp.where(keep, turned[t], turned[t + 1]) * ratio


def per_device(fields, lat_fraction, lon_fraction, lon_shift, departure_row, extents):
    rows, nfields, levels, lon = fields.shape
    chunks = [(k, f, lon * lane // parts, lon * width // parts) for k, f, lane, width, parts in CHUNKS]
    count = len(chunks)
    dma = pltpu.SemaphoreType.DMA
    mates = (NX - 1) + 1 + (NZ - 1) + (NY - 1)
    scratch = []
    for scheme, _, _, width in chunks:
        scratch += buffers_of(scheme, rows, levels, width)
    scratch += [
        pltpu.VMEM((nfields, rows, levels, lon), jnp.float32),
        pltpu.VMEM((NY * rows, 8, LANES), jnp.float32),
        pltpu.VMEM((7, 8, LANES), jnp.int32),
        pltpu.VMEM((7, 16, LANES), jnp.float32),
        pltpu.SMEM((7, 8, LANES), jnp.int32),
        pltpu.SMEM((7, 16, LANES), jnp.float32),
        pltpu.VMEM((4 + mates, 16, LANES), jnp.float32),
        dma((count,)), dma((count, 6)), dma((count, 6)), dma((12,)), dma((12,)), dma((2,)),
        dma((NY - 1,)), dma((NY - 1,)), dma((mates,)), dma((mates,)), dma((nfields,)),
    ]
    vmem = pl.BlockSpec(memory_space=pltpu.VMEM)
    column, ratio = pl.pallas_call(
        functools.partial(advect_kernel, rows, nfields, lon, chunks),
        out_shape=(
            jax.ShapeDtypeStruct(fields.shape, fields.dtype),
            jax.ShapeDtypeStruct((8, LANES), jnp.float32),
        ),
        in_specs=[vmem, vmem, vmem, vmem, pl.BlockSpec(memory_space=pl.ANY)],
        out_specs=(pl.BlockSpec(memory_space=pl.ANY), vmem),
        scratch_shapes=scratch,
        compiler_params=pltpu.CompilerParams(collective_id=0, has_side_effects=True),
    )(lat_fraction[None], lon_fraction[None], departure_row[None], extents, fields)
    block = pl.BlockSpec((ROWS_PER_STEP, nfields, levels, lon), lambda i: (i, 0, 0, 0))
    return pl.pallas_call(
        functools.partial(turn_kernel, nfields, lon),
        grid=(rows // ROWS_PER_STEP,),
        out_shape=jax.ShapeDtypeStruct(fields.shape, fields.dtype),
        in_specs=[pl.BlockSpec(memory_space=pltpu.SMEM), vmem, block],
        out_specs=block,
    )(lon_shift, ratio, column)


def solution(mesh):
    placed = (P("lat", None, "lev", None), P("lat"), P("lat"), P("lat"), P("lat"), P("lat", None))
    return jax.shard_map(
        per_device,
        mesh=mesh,
        in_specs=placed,
        out_specs=P("lat", None, "lev", None),
        check_vma=False,
    )
```

```python
import functools
import math

import jax
import jax.numpy as jnp
from jax import lax
from jax.experimental import pallas as pl
from jax.experimental.pallas import tpu as pltpu
from jax.sharding import PartitionSpec as P

MESH = pl.DeviceIdType.MESH
NY, NZ, NX = 4, 8, 4
LANES = 128
ROWS_PER_STEP = 2
CHUNKS = [('ring', 1, 1, 1, 2), ('pair', 2, 1, 1, 2), ('pair', 0, 1, 1, 2), ('column', 0, 0, 1, 2), ('column', 2, 0, 1, 2), ('column', 1, 0, 1, 2)]
ORDER = [0, 3, 2, 5, 3, 0, 4, 5, 2, 1, 3, 4, 5, 0, 2, 1, 4, 3, 2, 0, 1, 4, 5, 1]
MASS_AT = [2, 8, 15, 16, 23]


def cubic_weights(fraction):
    return [
        -fraction * (fraction - 1.0) * (fraction - 2.0) / 6.0,
        (fraction + 1.0) * (fraction - 1.0) * (fraction - 2.0) / 2.0,
        -(fraction + 1.0) * fraction * (fraction - 2.0) / 2.0,
        (fraction + 1.0) * fraction * (fraction - 1.0) / 6.0,
    ]


def buffers_of(scheme, rows, levels, width):
    half = rows // 2
    counts = {
        "ring": [NY * rows] + [rows] * 4,
        "column": [3 * rows] + [rows] * 3 + [half, rows - half] + [rows] * 2,
        "pair": [2 * rows] + [rows] * 8,
    }[scheme]
    return [pltpu.VMEM((n, levels, width), jnp.float32) for n in counts]


COPIES = {"ring": 6, "column": 6, "pair": 5}


def advect_kernel(rows, nfields, lon, chunks, *refs):
    refs = list(refs)
    lat_ref, lon_ref, departure_ref, extents_ref, fields_ref, out_ref, ratio_ref = refs[:7]
    scratch = refs[7:]
    count = len(chunks)
    bufs = []
    for chunk in chunks:
        n = len(buffers_of(chunk[0], rows, 8, LANES))
        bufs.append(scratch[:n])
        scratch = scratch[n:]
    (out_buf, sums, itab_all, ftab_all, itab, ftab, mass,
     load_sem, bulk_send, bulk_recv, tab_send, tab_recv, tab_local,
     sum_send, sum_recv, mass_send, mass_recv, out_sem) = scratch

    band = lax.axis_index("lat")
    core = lax.axis_index("lev")
    bands = NX * NZ * NY
    y = lax.rem(band, NY)
    z = lax.rem(lax.div(band, NY), NZ)
    x = lax.div(band, NY * NZ)
    base = band - y
    odd = lax.rem(y, 2)
    south = lax.div(y, 2)

    y_up, y_down = lax.rem(y + 1, NY), lax.rem(y + 3, NY)
    y_mates = [(base + lax.rem(y + s, NY), core) for s in (1, 2, 3)]
    z_mates = [(x * (NY * NZ) + lax.rem(z + s, NZ) * NY + y, core) for s in range(1, NZ)]
    x_mates = [(lax.rem(x + s, NX) * (NY * NZ) + z * NY + y, core) for s in range(1, NX)]
    c_mates = [(band, 1 - core)]
    up = (lax.rem(band + NY, bands), core)
    down = (lax.rem(band + bands - NY, bands), core)
    pair = (band + 1 - 2 * odd, core)
    cross = (base + 3 - y, core)
    toward = (lax.rem(band + bands - NY + 2 * NY * south, bands), core)
    diagonal = (lax.rem(base + 3 - y + bands - NY + 2 * NY * south, bands), core)
    partners = y_mates + z_mates + x_mates + c_mates + [up, down, diagonal]

    own_at = {"ring": y * rows, "column": rows, "pair": odd * rows}
    loads = [
        pltpu.make_async_copy(
            fields_ref.at[:, f, :, pl.ds(lane, width)],
            bufs[c][0].at[pl.ds(own_at[scheme], rows)],
            load_sem.at[c],
        )
        for c, (scheme, f, lane, width) in enumerate(chunks)
    ]
    loaded_first = []
    for c in ORDER + list(range(count)):
        if c not in loaded_first:
            loaded_first.append(c)
    for c in loaded_first:
        loads[c].start()

    barrier = pltpu.get_barrier_semaphore()
    for partner in partners:
        pl.semaphore_signal(barrier, inc=1, device_id=partner, device_id_type=MESH)

    first_row = band * rows
    low = first_row - extents_ref[0:1, 0:1] * rows + 1
    high = first_row + rows - 3 + extents_ref[0:1, 1:2] * rows
    start = jnp.minimum(jnp.maximum(departure_ref[...], low), high)
    start = jnp.minimum(jnp.maximum(start, 1), bands * rows - 3) - 1
    lat_w = cubic_weights(lat_ref[...])
    lon_w = cubic_weights(lon_ref[...])
    row_ids = first_row + lax.broadcasted_iota(jnp.int32, (1, rows), 1)
    area = jnp.cos(math.pi * (row_ids.astype(jnp.float32) + 0.5) / (bands * rows) - math.pi / 2.0)
    lon_total = lon_w[0] + lon_w[1] + lon_w[2] + lon_w[3]
    itab_all[0] = jnp.zeros((8, LANES), jnp.int32)
    ftab_all[0] = jnp.zeros((16, LANES), jnp.float32)
    itab_all[0, 0:1, 0:rows] = start
    for k, values in enumerate(lat_w + [area * lon_total] + lon_w + [area]):
        ftab_all[0, k:k + 1, 0:rows] = values

    for load in loads:
        load.wait()

    def row_sums(r, carry):
        pieces = []
        for f in range(nfields):
            total = None
            for c, (scheme, field, lane, width) in enumerate(chunks):
                if field != f:
                    continue
                block = bufs[c][0][own_at[scheme] + r]
                for t in range(width // LANES):
                    tile = block[:, t * LANES:(t + 1) * LANES]
                    total = tile if total is None else total + tile
            pieces.append(jnp.sum(total, axis=0, keepdims=True))
        pieces.append(jnp.zeros((8 - nfields, LANES), jnp.float32))
        sums[y * rows + r] = jnp.concatenate(pieces, axis=0)
        return carry

    lax.fori_loop(0, rows, row_sums, 0)
    pl.semaphore_wait(barrier, len(partners))

    def remote(src, dst, send_sem, recv_sem, target):
        return pltpu.make_async_remote_copy(
            src_ref=src, dst_ref=dst, send_sem=send_sem, recv_sem=recv_sem, device_id=target, device_id_type=MESH
        )

    table_routes = [(2, up), (1, down), (5, y_mates[0]), (4, y_mates[1]), (3, y_mates[2]), (6, diagonal)]
    tables = []
    for i, (slot, target) in enumerate(table_routes):
        for j, ref in enumerate((itab_all, ftab_all)):
            tables.append(remote(ref.at[0], ref.at[slot], tab_send.at[2 * i + j], tab_recv.at[2 * i + j], target))
    for copy in tables:
        copy.start()
    my_sums = sums.at[pl.ds(y * rows, rows)]
    sum_copies = [remote(my_sums, my_sums, sum_send.at[s], sum_recv.at[s], y_mates[s]) for s in range(NY - 1)]
    for copy in sum_copies:
        copy.start()

    def ring_spot(row):
        spot = row - base * rows
        return jnp.clip(spot, 0, NY * rows - 1), jnp.logical_and(spot >= 0, spot < NY * rows)

    def pair_spot(row):
        spot = row - (band - odd) * rows
        return jnp.clip(spot, 0, 2 * rows - 1), jnp.logical_and(spot >= 0, spot < 2 * rows)

    def column_spot(row):
        away = row - (band - NY) * rows
        block = (away >= NY * rows).astype(jnp.int32) + (away >= 2 * NY * rows).astype(jnp.int32)
        within = away - block * (NY * rows)
        return block * rows + jnp.clip(within, 0, rows - 1), jnp.logical_and(within >= 0, within < rows)

    def taps(spot_of, t, r):
        first = itab[t, 0, r]
        out = []
        for a in range(4):
            spot, inside = spot_of(first + a)
            out.append((spot, jnp.where(inside, ftab[t, a, r], 0.0)))
        return out

    def weighted(ref, spots):
        acc = None
        for spot, weight in spots:
            term = weight * ref[spot]
            acc = term if acc is None else acc + term
        return acc

    def partial_rows(spot_of, src, jobs):
        def one(r, carry):
            for t, dst, extra in jobs:
                acc = weighted(src, taps(spot_of, t, r))
                dst[r] = acc if extra is None else acc + extra[r]
            return carry

        lax.fori_loop(0, rows, one, 0)

    def add_rows(n, dst, dst_at, extra):
        def one(r, carry):
            dst[dst_at + r] = dst[dst_at + r] + extra[r]
            return carry

        lax.fori_loop(0, n, one, 0)

    ready = []

    def need_tables():
        if ready:
            return
        ready.append(True)
        for copy in tables:
            copy.wait_recv()
        moves = [
            pltpu.make_async_copy(itab_all, itab, tab_local.at[0]),
            pltpu.make_async_copy(ftab_all, ftab, tab_local.at[1]),
        ]
        for copy in moves:
            copy.start()
        for copy in moves:
            copy.wait()

    half = rows // 2
    finals = [None] * count

    def stages_of(c):
        scheme = chunks[c][0]
        b = bufs[c]
        send = [bulk_send.at[c, k] for k in range(COPIES[scheme])]
        recv = [bulk_recv.at[c, k] for k in range(COPIES[scheme])]

        def link(k, src, dst, target):
            return remote(src, dst, send[k], recv[k], target)

        if scheme == "ring":
            ring, send_up, send_down, recv_up, recv_down = b
            mine = ring.at[pl.ds(y * rows, rows)]
            from_down = ring.at[pl.ds(y_down * rows + half, rows - half)]
            from_up = ring.at[pl.ds(y_up * rows, half)]
            copies = [
                link(0, mine, mine, y_mates[0]), link(1, mine, mine, y_mates[2]),
                link(2, from_down, from_down, y_mates[0]), link(3, from_up, from_up, y_mates[2]),
                link(4, send_up, recv_up, up), link(5, send_down, recv_down, down),
            ]

            def stage0():
                copies[0].start()
                copies[1].start()

            def stage1():
                copies[0].wait_recv()
                copies[1].wait_recv()
                copies[2].start()
                copies[3].start()

            def stage2():
                copies[2].wait_recv()
                copies[3].wait_recv()
                need_tables()
                partial_rows(ring_spot, ring, [(1, send_up, None), (2, send_down, None)])
                copies[4].start()
                copies[5].start()

            def stage3():
                copies[4].wait_recv()
                copies[5].wait_recv()
                finals[c] = (ring_spot, ring, [recv_up, recv_down])

        elif scheme == "column":
            column, to_up, to_down, to_far, far_a, far_b, got_a, got_b = b
            mine = column.at[pl.ds(rows, rows)]
            copies = [
                link(0, mine, column.at[pl.ds(0, rows)], up), link(1, mine, column.at[pl.ds(2 * rows, rows)], down),
                link(2, to_far.at[pl.ds(0, half)], far_a, y_mates[0]),
                link(3, to_far.at[pl.ds(half, rows - half)], far_b, y_mates[2]),
                link(4, to_up, got_a, y_mates[0]), link(5, to_down, got_b, y_mates[2]),
            ]

            def stage0():
                copies[0].start()
                copies[1].start()

            def stage1():
                copies[0].wait_recv()
                copies[1].wait_recv()
                need_tables()
                partial_rows(column_spot, column, [(4, to_far, None)])
                copies[2].start()
                copies[3].start()
                partial_rows(column_spot, column, [(3, to_up, None), (5, to_down, None)])

            def stage2():
                copies[2].wait_recv()
                add_rows(half, to_up, 0, far_a)
                copies[4].start()
                copies[3].wait_recv()
                add_rows(rows - half, to_down, half, far_b)
                copies[5].start()

            def stage3():
                copies[4].wait_recv()
                copies[5].wait_recv()
                finals[c] = (column_spot, column, [got_a, got_b])

        else:
            both, to_up, to_down, to_diag, to_cross, from_down, from_up, passed, from_cross = b
            mine = both.at[pl.ds(odd * rows, rows)]
            copies = [
                link(0, mine, mine, pair), link(1, to_up, from_down, up), link(2, to_down, from_up, down),
                link(3, to_diag, passed, toward), link(4, to_cross, from_cross, cross),
            ]

            def stage0():
                copies[0].start()

            def stage1():
                copies[0].wait_recv()
                need_tables()
                partial_rows(pair_spot, both, [(6, to_diag, None)])
                copies[3].start()
                partial_rows(pair_spot, both, [(1, to_up, None), (2, to_down, None)])
                copies[1].start()
                copies[2].start()

            def stage2():
                copies[3].wait_recv()
                partial_rows(pair_spot, both, [(5 - 2 * odd, to_cross, passed)])
                copies[4].start()

            def stage3():
                copies[1].wait_recv()
                copies[2].wait_recv()
                copies[4].wait_recv()
                finals[c] = (pair_spot, both, [from_down, from_up, from_cross])

        return copies, [stage0, stage1, stage2, stage3]

    phases = [y_mates, z_mates, c_mates, x_mates]
    offsets = [0]
    for mates in phases:
        offsets.append(offsets[-1] + len(mates))
    mass_copies = []
    for k, mates in enumerate(phases):
        mass_copies.append([
            remote(mass.at[k], mass.at[len(phases) + offsets[k] + i], mass_send.at[offsets[k] + i],
                   mass_recv.at[offsets[k] + i], mate)
            for i, mate in enumerate(mates)
        ])

    def mass_step(step):
        if step == 0:
            need_tables()
            for copy in sum_copies:
                copy.wait_recv()

            def one(r, carry):
                before, after = carry
                before = before + ftab[0, 9, r] * sums[y * rows + r]
                for t in range(3):
                    after = after + ftab[t, 4, r] * weighted(sums, taps(ring_spot, t, r))
                return before, after

            zero = jnp.zeros((8, LANES), jnp.float32)
            before, after = lax.fori_loop(0, rows, one, (zero, zero))
            total = jnp.concatenate([before[0:4], after[0:4]], axis=0)
        else:
            k = step - 1
            total = mass[k]
            for i, copy in enumerate(mass_copies[k]):
                copy.wait_recv()
                total = total + mass[len(phases) + offsets[k] + i]
        if step < len(phases):
            mass[step] = total
            for copy in mass_copies[step]:
                copy.start()
        else:
            total = jnp.sum(total, axis=1, keepdims=True)
            ratio_ref[0:4] = jnp.broadcast_to(total[0:4] / total[4:8], (4, LANES))

    outs = [pltpu.make_async_copy(out_buf.at[f], out_ref.at[:, f], out_sem.at[f]) for f in range(nfields)]

    def finish(c):
        _, f, lane, width = chunks[c]
        spot_of, src, extras = finals[c]

        def one(r, carry):
            acc = weighted(src, taps(spot_of, 0, r))
            for extra in extras:
                acc = acc + extra[r]
            out_buf[f, r, :, lane:lane + width] = acc
            return carry

        lax.fori_loop(0, rows, one, 0)

    def filter_rows(f):
        def one(r, carry):
            column = out_buf[f, r]
            mixed = ftab[0, 5, r] * column
            for k in range(1, 4):
                mixed = mixed + ftab[0, 5 + k, r] * pltpu.roll(column, lon - k, 1)
            out_buf[f, r] = mixed
            return carry

        lax.fori_loop(0, rows, one, 0)
        outs[f].start()

    every = [stages_of(c) for c in range(count)]
    place = [0] * count
    left = [sum(1 for chunk in chunks if chunk[1] == f) for f in range(nfields)]
    mass_done = 0
    for i, c in enumerate(ORDER):
        every[c][1][place[c]]()
        place[c] += 1
        if place[c] == 4:
            finish(c)
            f = chunks[c][1]
            left[f] -= 1
            if left[f] == 0:
                filter_rows(f)
        while mass_done < len(MASS_AT) and MASS_AT[mass_done] == i:
            mass_step(mass_done)
            mass_done += 1

    for copies, _ in every:
        for copy in copies:
            copy.wait_send()
    for copy in tables + sum_copies:
        copy.wait_send()
    for group in mass_copies:
        for copy in group:
            copy.wait_send()
    for copy in outs:
        copy.wait()


def turn_kernel(nfields, lon, shift_ref, ratio_ref, column_ref, out_ref):
    lane_id = lax.broadcasted_iota(jnp.int32, (8, LANES), 1)
    tiles = lon // LANES
    for i in range(ROWS_PER_STEP):
        r = pl.program_id(0) * ROWS_PER_STEP + i
        begin = shift_ref[r] - 1
        begin = jnp.where(begin < 0, begin + lon, begin)
        whole = lax.shift_right_logical(begin, 7)
        rest = jnp.bitwise_and(begin, LANES - 1)
        turn = jnp.bitwise_and(LANES - rest, LANES - 1)
        keep = lane_id < (LANES - rest)
        spots = []
        for t in range(tiles + 1):
            spot = whole + t
            spot = jnp.where(spot >= tiles, spot - tiles, spot)
            spots.append(pl.multiple_of(spot * LANES, LANES))
        for f in range(nfields):
            ratio = jnp.broadcast_to(ratio_ref[f:f + 1, :], (8, LANES))
            turned = [pltpu.roll(column_ref[i, f, :, pl.ds(spot, LANES)], turn, 1) for spot in spots]
            for t in range(tiles):
                out_ref[i, f, :, t * LANES:(t + 1) * LANES] = jnp.where(keep, turned[t], turned[t + 1]) * ratio


def per_device(fields, lat_fraction, lon_fraction, lon_shift, departure_row, extents):
    rows, nfields, levels, lon = fields.shape
    chunks = [(k, f, lon * lane // parts, lon * width // parts) for k, f, lane, width, parts in CHUNKS]
    count = len(chunks)
    dma = pltpu.SemaphoreType.DMA
    mates = (NX - 1) + 1 + (NZ - 1) + (NY - 1)
    scratch = []
    for scheme, _, _, width in chunks:
        scratch += buffers_of(scheme, rows, levels, width)
    scratch += [
        pltpu.VMEM((nfields, rows, levels, lon), jnp.float32),
        pltpu.VMEM((NY * rows, 8, LANES), jnp.float32),
        pltpu.VMEM((7, 8, LANES), jnp.int32),
        pltpu.VMEM((7, 16, LANES), jnp.float32),
        pltpu.SMEM((7, 8, LANES), jnp.int32),
        pltpu.SMEM((7, 16, LANES), jnp.float32),
        pltpu.VMEM((4 + mates, 8, LANES), jnp.float32),
        dma((count,)), dma((count, 6)), dma((count, 6)), dma((12,)), dma((12,)), dma((2,)),
        dma((NY - 1,)), dma((NY - 1,)), dma((mates,)), dma((mates,)), dma((nfields,)),
    ]
    vmem = pl.BlockSpec(memory_space=pltpu.VMEM)
    column, ratio = pl.pallas_call(
        functools.partial(advect_kernel, rows, nfields, lon, chunks),
        out_shape=(
            jax.ShapeDtypeStruct(fields.shape, fields.dtype),
            jax.ShapeDtypeStruct((4, LANES), jnp.float32),
        ),
        in_specs=[vmem, vmem, vmem, vmem, pl.BlockSpec(memory_space=pl.ANY)],
        out_specs=(pl.BlockSpec(memory_space=pl.ANY), vmem),
        scratch_shapes=scratch,
        compiler_params=pltpu.CompilerParams(collective_id=0, has_side_effects=True),
    )(lat_fraction[None], lon_fraction[None], departure_row[None], extents, fields)
    block = pl.BlockSpec((ROWS_PER_STEP, nfields, levels, lon), lambda i: (i, 0, 0, 0))
    return pl.pallas_call(
        functools.partial(turn_kernel, nfields, lon),
        grid=(rows // ROWS_PER_STEP,),
        out_shape=jax.ShapeDtypeStruct(fields.shape, fields.dtype),
        in_specs=[pl.BlockSpec(memory_space=pltpu.SMEM), vmem, block],
        out_specs=block,
    )(lon_shift, ratio, column)


def solution(mesh):
    placed = (P("lat", None, "lev", None), P("lat"), P("lat"), P("lat"), P("lat"), P("lat", None))
    return jax.shard_map(
        per_device,
        mesh=mesh,
        in_specs=placed,
        out_specs=P("lat", None, "lev", None),
        check_vma=False,
    )
```

```python
import functools
import math

import jax
import jax.numpy as jnp
from jax import lax
from jax.experimental import pallas as pl
from jax.experimental.pallas import tpu as pltpu
from jax.sharding import PartitionSpec as P

MESH = pl.DeviceIdType.MESH
NY, NZ, NX = 4, 8, 4
LANES = 128
ROWS_PER_STEP = 2
KERNEL_VMEM = 50 * 1024 * 1024
CHUNKS = [('ring', 1, 1, 1, 2), ('pair', 2, 1, 1, 2), ('pair', 0, 1, 1, 2), ('column', 0, 0, 1, 2), ('column', 2, 0, 1, 2), ('column', 1, 0, 1, 2)]
ORDER = [0, 3, 2, 5, 3, 0, 4, 5, 2, 1, 3, 4, 5, 0, 2, 1, 4, 3, 2, 0, 1, 4, 5, 1]
MASS_AT = [2, 8, 15, 16, 23]


def cubic_weights(fraction):
    return [
        -fraction * (fraction - 1.0) * (fraction - 2.0) / 6.0,
        (fraction + 1.0) * (fraction - 1.0) * (fraction - 2.0) / 2.0,
        -(fraction + 1.0) * fraction * (fraction - 2.0) / 2.0,
        (fraction + 1.0) * fraction * (fraction - 1.0) / 6.0,
    ]


def buffers_of(scheme, rows, levels, width):
    half = rows // 2
    counts = {
        "ring": [NY * rows] + [rows] * 4,
        "column": [3 * rows] + [rows] * 3 + [half, rows - half] + [rows] * 2,
        "pair": [2 * rows] + [rows] * 8,
    }[scheme]
    return [pltpu.VMEM((n, levels, width), jnp.float32) for n in counts]


COPIES = {"ring": 6, "column": 6, "pair": 5}


def advect_kernel(rows, nfields, lon, chunks, *refs):
    refs = list(refs)
    fractions_ref, numbers_ref, fields_ref, out_ref, ratio_ref = refs[:5]
    scratch = refs[5:]
    count = len(chunks)
    bufs = []
    for chunk in chunks:
        n = len(buffers_of(chunk[0], rows, 8, LANES))
        bufs.append(scratch[:n])
        scratch = scratch[n:]
    (sums, itab_all, ftab_all, itab, ftab, mass,
     load_sem, bulk_send, bulk_recv, tab_send, tab_recv, tab_local,
     sum_send, sum_recv, mass_send, mass_recv, out_sem) = scratch

    band = lax.axis_index("lat")
    core = lax.axis_index("lev")
    bands = NX * NZ * NY
    y = lax.rem(band, NY)
    z = lax.rem(lax.div(band, NY), NZ)
    x = lax.div(band, NY * NZ)
    base = band - y
    odd = lax.rem(y, 2)
    south = lax.div(y, 2)

    y_up, y_down = lax.rem(y + 1, NY), lax.rem(y + 3, NY)
    y_mates = [(base + lax.rem(y + s, NY), core) for s in (1, 2, 3)]
    z_mates = [(x * (NY * NZ) + lax.rem(z + s, NZ) * NY + y, core) for s in range(1, NZ)]
    x_mates = [(lax.rem(x + s, NX) * (NY * NZ) + z * NY + y, core) for s in range(1, NX)]
    c_mates = [(band, 1 - core)]
    up = (lax.rem(band + NY, bands), core)
    down = (lax.rem(band + bands - NY, bands), core)
    pair = (band + 1 - 2 * odd, core)
    cross = (base + 3 - y, core)
    toward = (lax.rem(band + bands - NY + 2 * NY * south, bands), core)
    diagonal = (lax.rem(base + 3 - y + bands - NY + 2 * NY * south, bands), core)
    partners = y_mates + z_mates + x_mates + c_mates + [up, down, diagonal]

    own_at = {"ring": y * rows, "column": rows, "pair": odd * rows}
    loads = [
        pltpu.make_async_copy(
            fields_ref.at[:, f, :, pl.ds(lane, width)],
            bufs[c][0].at[pl.ds(own_at[scheme], rows)],
            load_sem.at[c],
        )
        for c, (scheme, f, lane, width) in enumerate(chunks)
    ]
    loaded_first = []
    for c in ORDER + list(range(count)):
        if c not in loaded_first:
            loaded_first.append(c)
    for c in loaded_first:
        loads[c].start()

    barrier = pltpu.get_barrier_semaphore()
    for partner in partners:
        pl.semaphore_signal(barrier, inc=1, device_id=partner, device_id_type=MESH)

    first_row = band * rows
    low = first_row - numbers_ref[0:1, rows:rows + 1] * rows + 1
    high = first_row + rows - 3 + numbers_ref[0:1, rows + 1:rows + 2] * rows
    start = jnp.minimum(jnp.maximum(numbers_ref[0:1, 0:rows], low), high)
    start = jnp.minimum(jnp.maximum(start, 1), bands * rows - 3) - 1
    lat_w = cubic_weights(fractions_ref[0:1])
    lon_w = cubic_weights(fractions_ref[1:2])
    row_ids = first_row + lax.broadcasted_iota(jnp.int32, (1, rows), 1)
    area = jnp.cos(math.pi * (row_ids.astype(jnp.float32) + 0.5) / (bands * rows) - math.pi / 2.0)
    lon_total = lon_w[0] + lon_w[1] + lon_w[2] + lon_w[3]
    itab_all[0] = jnp.zeros((8, LANES), jnp.int32)
    ftab_all[0] = jnp.zeros((16, LANES), jnp.float32)
    itab_all[0, 0:1, 0:rows] = start
    for k, values in enumerate(lat_w + [area * lon_total] + lon_w + [area]):
        ftab_all[0, k:k + 1, 0:rows] = values

    for load in loads:
        load.wait()

    def row_sums(r, carry):
        pieces = []
        for f in range(nfields):
            total = None
            for c, (scheme, field, lane, width) in enumerate(chunks):
                if field != f:
                    continue
                block = bufs[c][0][own_at[scheme] + r]
                for t in range(width // LANES):
                    tile = block[:, t * LANES:(t + 1) * LANES]
                    total = tile if total is None else total + tile
            pieces.append(jnp.sum(total, axis=0, keepdims=True))
        pieces.append(jnp.zeros((8 - nfields, LANES), jnp.float32))
        sums[y * rows + r] = jnp.concatenate(pieces, axis=0)
        return carry

    lax.fori_loop(0, rows, row_sums, 0)
    pl.semaphore_wait(barrier, len(partners))

    def remote(src, dst, send_sem, recv_sem, target):
        return pltpu.make_async_remote_copy(
            src_ref=src, dst_ref=dst, send_sem=send_sem, recv_sem=recv_sem, device_id=target, device_id_type=MESH
        )

    table_routes = [(2, up), (1, down), (5, y_mates[0]), (4, y_mates[1]), (3, y_mates[2]), (6, diagonal)]
    tables = []
    for i, (slot, target) in enumerate(table_routes):
        for j, ref in enumerate((itab_all, ftab_all)):
            tables.append(remote(ref.at[0], ref.at[slot], tab_send.at[2 * i + j], tab_recv.at[2 * i + j], target))
    for copy in tables:
        copy.start()
    my_sums = sums.at[pl.ds(y * rows, rows)]
    sum_copies = [remote(my_sums, my_sums, sum_send.at[s], sum_recv.at[s], y_mates[s]) for s in range(NY - 1)]
    for copy in sum_copies:
        copy.start()

    def ring_spot(row):
        spot = row - base * rows
        return jnp.clip(spot, 0, NY * rows - 1), jnp.logical_and(spot >= 0, spot < NY * rows)

    def pair_spot(row):
        spot = row - (band - odd) * rows
        return jnp.clip(spot, 0, 2 * rows - 1), jnp.logical_and(spot >= 0, spot < 2 * rows)

    def column_spot(row):
        away = row - (band - NY) * rows
        block = (away >= NY * rows).astype(jnp.int32) + (away >= 2 * NY * rows).astype(jnp.int32)
        within = away - block * (NY * rows)
        return block * rows + jnp.clip(within, 0, rows - 1), jnp.logical_and(within >= 0, within < rows)

    def taps(spot_of, t, r):
        first = itab[t, 0, r]
        out = []
        for a in range(4):
            spot, inside = spot_of(first + a)
            out.append((spot, jnp.where(inside, ftab[t, a, r], 0.0)))
        return out

    def weighted(ref, spots):
        acc = None
        for spot, weight in spots:
            term = weight * ref[spot]
            acc = term if acc is None else acc + term
        return acc

    def partial_rows(spot_of, src, jobs):
        def one(r, carry):
            for t, dst, extra in jobs:
                acc = weighted(src, taps(spot_of, t, r))
                dst[r] = acc if extra is None else acc + extra[r]
            return carry

        lax.fori_loop(0, rows, one, 0)

    def add_rows(n, dst, dst_at, extra):
        def one(r, carry):
            dst[dst_at + r] = dst[dst_at + r] + extra[r]
            return carry

        lax.fori_loop(0, n, one, 0)

    ready = []

    def need_tables():
        if ready:
            return
        ready.append(True)
        for copy in tables:
            copy.wait_recv()
        moves = [
            pltpu.make_async_copy(itab_all, itab, tab_local.at[0]),
            pltpu.make_async_copy(ftab_all, ftab, tab_local.at[1]),
        ]
        for copy in moves:
            copy.start()
        for copy in moves:
            copy.wait()

    half = rows // 2
    finals = [None] * count

    def stages_of(c):
        scheme = chunks[c][0]
        b = bufs[c]
        send = [bulk_send.at[c, k] for k in range(COPIES[scheme])]
        recv = [bulk_recv.at[c, k] for k in range(COPIES[scheme])]

        def link(k, src, dst, target):
            return remote(src, dst, send[k], recv[k], target)

        if scheme == "ring":
            ring, send_up, send_down, recv_up, recv_down = b
            mine = ring.at[pl.ds(y * rows, rows)]
            from_down = ring.at[pl.ds(y_down * rows + half, rows - half)]
            from_up = ring.at[pl.ds(y_up * rows, half)]
            copies = [
                link(0, mine, mine, y_mates[0]), link(1, mine, mine, y_mates[2]),
                link(2, from_down, from_down, y_mates[0]), link(3, from_up, from_up, y_mates[2]),
                link(4, send_up, recv_up, up), link(5, send_down, recv_down, down),
            ]

            def stage0():
                copies[0].start()
                copies[1].start()

            def stage1():
                copies[0].wait_recv()
                copies[1].wait_recv()
                copies[2].start()
                copies[3].start()

            def stage2():
                copies[2].wait_recv()
                copies[3].wait_recv()
                need_tables()
                partial_rows(ring_spot, ring, [(1, send_up, None), (2, send_down, None)])
                copies[4].start()
                copies[5].start()

            def stage3():
                copies[4].wait_recv()
                copies[5].wait_recv()
                finals[c] = (ring_spot, ring, [recv_up, recv_down])

        elif scheme == "column":
            column, to_up, to_down, to_far, far_a, far_b, got_a, got_b = b
            mine = column.at[pl.ds(rows, rows)]
            copies = [
                link(0, mine, column.at[pl.ds(0, rows)], up), link(1, mine, column.at[pl.ds(2 * rows, rows)], down),
                link(2, to_far.at[pl.ds(0, half)], far_a, y_mates[0]),
                link(3, to_far.at[pl.ds(half, rows - half)], far_b, y_mates[2]),
                link(4, to_up, got_a, y_mates[0]), link(5, to_down, got_b, y_mates[2]),
            ]

            def stage0():
                copies[0].start()
                copies[1].start()

            def stage1():
                copies[0].wait_recv()
                copies[1].wait_recv()
                need_tables()
                partial_rows(column_spot, column, [(4, to_far, None)])
                copies[2].start()
                copies[3].start()
                partial_rows(column_spot, column, [(3, to_up, None), (5, to_down, None)])

            def stage2():
                copies[2].wait_recv()
                add_rows(half, to_up, 0, far_a)
                copies[4].start()
                copies[3].wait_recv()
                add_rows(rows - half, to_down, half, far_b)
                copies[5].start()

            def stage3():
                copies[4].wait_recv()
                copies[5].wait_recv()
                finals[c] = (column_spot, column, [got_a, got_b])

        else:
            both, to_up, to_down, to_diag, to_cross, from_down, from_up, passed, from_cross = b
            mine = both.at[pl.ds(odd * rows, rows)]
            copies = [
                link(0, mine, mine, pair), link(1, to_up, from_down, up), link(2, to_down, from_up, down),
                link(3, to_diag, passed, toward), link(4, to_cross, from_cross, cross),
            ]

            def stage0():
                copies[0].start()

            def stage1():
                copies[0].wait_recv()
                need_tables()
                partial_rows(pair_spot, both, [(6, to_diag, None)])
                copies[3].start()
                partial_rows(pair_spot, both, [(1, to_up, None), (2, to_down, None)])
                copies[1].start()
                copies[2].start()

            def stage2():
                copies[3].wait_recv()
                partial_rows(pair_spot, both, [(5 - 2 * odd, to_cross, passed)])
                copies[4].start()

            def stage3():
                copies[1].wait_recv()
                copies[2].wait_recv()
                copies[4].wait_recv()
                finals[c] = (pair_spot, both, [from_down, from_up, from_cross])

        return copies, [stage0, stage1, stage2, stage3]

    phases = [y_mates, z_mates, c_mates, x_mates]
    offsets = [0]
    for mates in phases:
        offsets.append(offsets[-1] + len(mates))
    mass_copies = []
    for k, mates in enumerate(phases):
        mass_copies.append([
            remote(mass.at[k], mass.at[len(phases) + offsets[k] + i], mass_send.at[offsets[k] + i],
                   mass_recv.at[offsets[k] + i], mate)
            for i, mate in enumerate(mates)
        ])

    def mass_step(step):
        if step == 0:
            need_tables()
            for copy in sum_copies:
                copy.wait_recv()

            def one(r, carry):
                before, after = carry
                before = before + ftab[0, 9, r] * sums[y * rows + r]
                for t in range(3):
                    after = after + ftab[t, 4, r] * weighted(sums, taps(ring_spot, t, r))
                return before, after

            zero = jnp.zeros((8, LANES), jnp.float32)
            before, after = lax.fori_loop(0, rows, one, (zero, zero))
            total = jnp.concatenate([before[0:4], after[0:4]], axis=0)
        else:
            k = step - 1
            total = mass[k]
            for i, copy in enumerate(mass_copies[k]):
                copy.wait_recv()
                total = total + mass[len(phases) + offsets[k] + i]
        if step < len(phases):
            mass[step] = total
            for copy in mass_copies[step]:
                copy.start()
        else:
            total = jnp.sum(total, axis=1, keepdims=True)
            ratio_ref[0:4] = jnp.broadcast_to(total[0:4] / total[4:8], (4, LANES))


    def finish(c):
        _, f, lane, width = chunks[c]
        spot_of, src, extras = finals[c]

        def one(r, carry):
            acc = weighted(src, taps(spot_of, 0, r))
            for extra in extras:
                acc = acc + extra[r]
            out_ref[r, f, :, lane:lane + width] = acc
            return carry

        lax.fori_loop(0, rows, one, 0)

    def filter_rows(f):
        def one(i, carry):
            for r in (2 * i, 2 * i + 1):
                column = out_ref[r, f]
                mixed = ftab[0, 5, r] * column
                for k in range(1, 4):
                    mixed = mixed + ftab[0, 5 + k, r] * pltpu.roll(column, lon - k, 1)
                out_ref[r, f] = mixed
            return carry

        lax.fori_loop(0, rows // 2, one, 0)

    every = [stages_of(c) for c in range(count)]
    place = [0] * count
    left = [sum(1 for chunk in chunks if chunk[1] == f) for f in range(nfields)]
    mass_done = 0
    for i, c in enumerate(ORDER):
        every[c][1][place[c]]()
        place[c] += 1
        if place[c] == 4:
            finish(c)
            f = chunks[c][1]
            left[f] -= 1
            if left[f] == 0:
                filter_rows(f)
        while mass_done < len(MASS_AT) and MASS_AT[mass_done] == i:
            mass_step(mass_done)
            mass_done += 1

    for copies, _ in every:
        for copy in copies:
            copy.wait_send()
    for copy in tables + sum_copies:
        copy.wait_send()
    for group in mass_copies:
        for copy in group:
            copy.wait_send()


def turn_kernel(nfields, lon, shift_ref, ratio_ref, column_ref, out_ref):
    lane_id = lax.broadcasted_iota(jnp.int32, (8, LANES), 1)
    tiles = lon // LANES
    for i in range(ROWS_PER_STEP):
        r = pl.program_id(0) * ROWS_PER_STEP + i
        begin = shift_ref[r] - 1
        begin = jnp.where(begin < 0, begin + lon, begin)
        whole = lax.shift_right_logical(begin, 7)
        rest = jnp.bitwise_and(begin, LANES - 1)
        turn = jnp.bitwise_and(LANES - rest, LANES - 1)
        keep = lane_id < (LANES - rest)
        spots = []
        for t in range(tiles + 1):
            spot = whole + t
            spot = jnp.where(spot >= tiles, spot - tiles, spot)
            spots.append(pl.multiple_of(spot * LANES, LANES))
        for f in range(nfields):
            ratio = jnp.broadcast_to(ratio_ref[f:f + 1, :], (8, LANES))
            turned = [pltpu.roll(column_ref[r, f, :, pl.ds(spot, LANES)], turn, 1) for spot in spots]
            for t in range(tiles):
                out_ref[i, f, :, t * LANES:(t + 1) * LANES] = jnp.where(keep, turned[t], turned[t + 1]) * ratio


def per_device(fields, lat_fraction, lon_fraction, lon_shift, departure_row, extents):
    rows, nfields, levels, lon = fields.shape
    chunks = [(k, f, lon * lane // parts, lon * width // parts) for k, f, lane, width, parts in CHUNKS]
    count = len(chunks)
    dma = pltpu.SemaphoreType.DMA
    mates = (NX - 1) + 1 + (NZ - 1) + (NY - 1)
    scratch = []
    for scheme, _, _, width in chunks:
        scratch += buffers_of(scheme, rows, levels, width)
    scratch += [
        pltpu.VMEM((NY * rows, 8, LANES), jnp.float32),
        pltpu.VMEM((7, 8, LANES), jnp.int32),
        pltpu.VMEM((7, 16, LANES), jnp.float32),
        pltpu.SMEM((7, 8, LANES), jnp.int32),
        pltpu.SMEM((7, 16, LANES), jnp.float32),
        pltpu.VMEM((4 + mates, 8, LANES), jnp.float32),
        dma((count,)), dma((count, 6)), dma((count, 6)), dma((12,)), dma((12,)), dma((2,)),
        dma((NY - 1,)), dma((NY - 1,)), dma((mates,)), dma((mates,)), dma((nfields,)),
    ]
    vmem = pl.BlockSpec(memory_space=pltpu.VMEM)
    column, ratio = pl.pallas_call(
        functools.partial(advect_kernel, rows, nfields, lon, chunks),
        out_shape=(
            jax.ShapeDtypeStruct(fields.shape, fields.dtype),
            jax.ShapeDtypeStruct((4, LANES), jnp.float32),
        ),
        in_specs=[vmem, vmem, pl.BlockSpec(memory_space=pl.ANY)],
        out_specs=(vmem, vmem),
        scratch_shapes=scratch,
        compiler_params=pltpu.CompilerParams(collective_id=0, has_side_effects=True, vmem_limit_bytes=KERNEL_VMEM),
    )(jnp.stack([lat_fraction, lon_fraction]), jnp.concatenate([departure_row[None], extents], axis=1), fields)
    block = pl.BlockSpec((ROWS_PER_STEP, nfields, levels, lon), lambda i: (i, 0, 0, 0))
    return pl.pallas_call(
        functools.partial(turn_kernel, nfields, lon),
        grid=(rows // ROWS_PER_STEP,),
        out_shape=jax.ShapeDtypeStruct(fields.shape, fields.dtype),
        in_specs=[pl.BlockSpec(memory_space=pltpu.SMEM), vmem, vmem],
        out_specs=block,
        compiler_params=pltpu.CompilerParams(vmem_limit_bytes=16 * 1024 * 1024),
    )(lon_shift, ratio, column)


def solution(mesh):
    placed = (P("lat", None, "lev", None), P("lat"), P("lat"), P("lat"), P("lat"), P("lat", None))
    return jax.shard_map(
        per_device,
        mesh=mesh,
        in_specs=placed,
        out_specs=P("lat", None, "lev", None),
        check_vma=False,
    )
```

```python
import functools
import math

import jax
import jax.numpy as jnp
from jax import lax
from jax.experimental import pallas as pl
from jax.experimental.pallas import tpu as pltpu
from jax.sharding import PartitionSpec as P

MESH = pl.DeviceIdType.MESH
NY, NZ, NX = 4, 8, 4
LANES = 128
ROWS_PER_STEP = 2
KERNEL_VMEM = 50 * 1024 * 1024
CHUNKS = [('pair', 0, 0, 5), ('mirror', 0, 5, 5), ('pair', 0, 10, 10), ('ring', 1, 0, 15), ('column', 1, 15, 5), ('mirror', 2, 0, 10), ('ring', 2, 10, 5), ('column', 2, 15, 5)]
ORDER = [4, 0, 1, 2, 5, 7, 1, 3, 0, 1, 5, 6, 2, 0, 3, 4, 7, 2, 6, 5, 4, 0, 3, 6, 2, 7, 3, 5, 1, 4, 6, 7]
MASS_AT = [3, 11, 24, 25, 31]


def cubic_weights(fraction):
    return [
        -fraction * (fraction - 1.0) * (fraction - 2.0) / 6.0,
        (fraction + 1.0) * (fraction - 1.0) * (fraction - 2.0) / 2.0,
        -(fraction + 1.0) * fraction * (fraction - 2.0) / 2.0,
        (fraction + 1.0) * fraction * (fraction - 1.0) / 6.0,
    ]


def buffers_of(scheme, rows, levels, width):
    half = rows // 2
    counts = {
        "ring": [NY * rows] + [rows] * 4,
        "column": [3 * rows] + [rows] * 3 + [half, rows - half] + [rows] * 2,
        "pair": [2 * rows] + [rows] * 8,
        "mirror": [2 * rows] + [rows] * 8,
    }[scheme]
    return [pltpu.VMEM((n, levels, width), jnp.float32) for n in counts]


COPIES = {"ring": 6, "column": 6, "pair": 5, "mirror": 5}


class Guarded:
    def __init__(self, copy, sends, gets):
        self.copy, self.sends, self.gets = copy, sends, gets

    def start(self):
        pl.when(self.sends)(lambda: self.copy.start())

    def wait_recv(self):
        pl.when(self.gets)(lambda: self.copy.wait_recv())

    def wait_send(self):
        pl.when(self.sends)(lambda: self.copy.wait_send())


def advect_kernel(rows, nfields, lon, chunks, *refs):
    refs = list(refs)
    fractions_ref, numbers_ref, fields_ref, out_ref, ratio_ref = refs[:5]
    scratch = refs[5:]
    count = len(chunks)
    bufs = []
    for chunk in chunks:
        n = len(buffers_of(chunk[0], rows, 8, LANES))
        bufs.append(scratch[:n])
        scratch = scratch[n:]
    (sums, itab_all, ftab_all, itab, ftab, mass,
     load_sem, bulk_send, bulk_recv, tab_send, tab_recv, tab_local,
     sum_send, sum_recv, mass_send, mass_recv, out_sem) = scratch

    band = lax.axis_index("lat")
    core = lax.axis_index("lev")
    bands = NX * NZ * NY
    y = lax.rem(band, NY)
    z = lax.rem(lax.div(band, NY), NZ)
    x = lax.div(band, NY * NZ)
    base = band - y
    odd = lax.rem(y, 2)
    south = lax.div(y, 2)

    y_up, y_down = lax.rem(y + 1, NY), lax.rem(y + 3, NY)
    y_mates = [(base + lax.rem(y + s, NY), core) for s in (1, 2, 3)]
    z_mates = [(x * (NY * NZ) + lax.rem(z + s, NZ) * NY + y, core) for s in range(1, NZ)]
    x_mates = [(lax.rem(x + s, NX) * (NY * NZ) + z * NY + y, core) for s in range(1, NX)]
    c_mates = [(band, 1 - core)]
    up = (lax.rem(band + NY, bands), core)
    down = (lax.rem(band + bands - NY, bands), core)
    pair = (band + 1 - 2 * odd, core)
    cross = (base + 3 - y, core)
    toward = (lax.rem(band + bands - NY + 2 * NY * south, bands), core)
    diagonal = (lax.rem(base + 3 - y + bands - NY + 2 * NY * south, bands), core)
    outer = jnp.logical_or(y == 0, y == NY - 1)
    inner = jnp.logical_not(outer)
    toward_main = (lax.rem(band + NY + bands - 2 * NY * south, bands), core)
    behind = toward
    before = (lax.rem(band + 1 - 2 * odd + NY + bands - 2 * NY * south, bands), core)
    after = (lax.rem(band + 1 - 2 * odd + bands - NY + 2 * NY * south, bands), core)
    partners = y_mates + z_mates + x_mates + c_mates + [up, down, diagonal, before, after]

    own_at = {"ring": y * rows, "column": rows, "pair": odd * rows, "mirror": south * rows}
    loads = [
        pltpu.make_async_copy(
            fields_ref.at[:, f, :, pl.ds(lane, width)],
            bufs[c][0].at[pl.ds(own_at[scheme], rows)],
            load_sem.at[c],
        )
        for c, (scheme, f, lane, width) in enumerate(chunks)
    ]
    loaded_first = []
    for c in ORDER + list(range(count)):
        if c not in loaded_first:
            loaded_first.append(c)
    for c in loaded_first:
        loads[c].start()

    can_up, can_down = band + NY < bands, band >= NY
    by_half = lambda north, south_side: jnp.logical_or(
        jnp.logical_and(south == 0, north), jnp.logical_and(south == 1, south_side)
    )
    to_up_down, to_down_up = by_half(can_up, can_down), by_half(can_down, can_up)

    barrier = pltpu.get_barrier_semaphore()
    for partner in partners:
        pl.semaphore_signal(barrier, inc=1, device_id=partner, device_id_type=MESH)

    def clear(ref, first, n):
        def one(r, carry):
            ref[first + r] = jnp.zeros(ref.shape[1:], jnp.float32)
            return carry

        lax.fori_loop(0, n, one, 0)

    for at_end, side in ((jnp.logical_not(can_down), 0), (jnp.logical_not(can_up), 1)):

        @pl.when(at_end)
        def _(side=side):
            for b, chunk in zip(bufs, chunks):
                if chunk[0] == "ring":
                    clear(b[3 + side], 0, rows)
                elif chunk[0] == "column":
                    clear(b[0], 2 * side * rows, rows)
                elif chunk[0] == "pair":
                    clear(b[5 + side], 0, rows)
                    pl.when(south == 1 - side)(lambda b=b: clear(b[7], 0, rows))
                else:
                    pl.when(south == side)(lambda b=b: clear(b[5], 0, rows))
                    pl.when(south == side)(lambda b=b: clear(b[7], 0, rows))
                    pl.when(south == 1 - side)(lambda b=b: clear(b[6], 0, rows))

    first_row = band * rows
    low = first_row - numbers_ref[0:1, rows:rows + 1] * rows + 1
    high = first_row + rows - 3 + numbers_ref[0:1, rows + 1:rows + 2] * rows
    start = jnp.minimum(jnp.maximum(numbers_ref[0:1, 0:rows], low), high)
    start = jnp.minimum(jnp.maximum(start, 1), bands * rows - 3) - 1
    lat_w = cubic_weights(fractions_ref[0:1])
    lon_w = cubic_weights(fractions_ref[1:2])
    row_ids = first_row + lax.broadcasted_iota(jnp.int32, (1, rows), 1)
    area = jnp.cos(math.pi * (row_ids.astype(jnp.float32) + 0.5) / (bands * rows) - math.pi / 2.0)
    lon_total = lon_w[0] + lon_w[1] + lon_w[2] + lon_w[3]
    itab_all[0] = jnp.zeros((8, LANES), jnp.int32)
    ftab_all[0] = jnp.zeros((16, LANES), jnp.float32)
    itab_all[0, 0:1, 0:rows] = start
    for k, values in enumerate(lat_w + [area * lon_total] + lon_w + [area]):
        ftab_all[0, k:k + 1, 0:rows] = values

    for load in loads:
        load.wait()

    def row_sums(r, carry):
        pieces = []
        for f in range(nfields):
            total = None
            for c, (scheme, field, lane, width) in enumerate(chunks):
                if field != f:
                    continue
                block = bufs[c][0][own_at[scheme] + r]
                for t in range(width // LANES):
                    tile = block[:, t * LANES:(t + 1) * LANES]
                    total = tile if total is None else total + tile
            pieces.append(jnp.sum(total, axis=0, keepdims=True))
        pieces.append(jnp.zeros((8 - nfields, LANES), jnp.float32))
        sums[y * rows + r] = jnp.concatenate(pieces, axis=0)
        return carry

    lax.fori_loop(0, rows, row_sums, 0)
    pl.semaphore_wait(barrier, len(partners))

    def remote(src, dst, send_sem, recv_sem, target):
        return pltpu.make_async_remote_copy(
            src_ref=src, dst_ref=dst, send_sem=send_sem, recv_sem=recv_sem, device_id=target, device_id_type=MESH
        )

    table_routes = [(2, up), (1, down), (5, y_mates[0]), (4, y_mates[1]), (3, y_mates[2]), (6, diagonal), (7, after)]
    tables = []
    for i, (slot, target) in enumerate(table_routes):
        for j, ref in enumerate((itab_all, ftab_all)):
            tables.append(remote(ref.at[0], ref.at[slot], tab_send.at[2 * i + j], tab_recv.at[2 * i + j], target))
    for copy in tables:
        copy.start()
    my_sums = sums.at[pl.ds(y * rows, rows)]
    sum_copies = [remote(my_sums, my_sums, sum_send.at[s], sum_recv.at[s], y_mates[s]) for s in range(NY - 1)]
    for copy in sum_copies:
        copy.start()

    def ring_spot(row):
        spot = row - base * rows
        return jnp.clip(spot, 0, NY * rows - 1), jnp.logical_and(spot >= 0, spot < NY * rows)

    def pair_spot(row):
        spot = row - (band - odd) * rows
        return jnp.clip(spot, 0, 2 * rows - 1), jnp.logical_and(spot >= 0, spot < 2 * rows)

    mirror_low = (base + jnp.where(outer, 0, 1)) * rows
    mirror_high = (base + jnp.where(outer, 3, 2)) * rows
    mirror_far = (band + NY - 2 * NY * south) * rows

    def mirror_spot(row):
        low_at, high_at = row - mirror_low, row - mirror_high
        in_low = jnp.logical_and(low_at >= 0, low_at < rows)
        in_high = jnp.logical_and(high_at >= 0, high_at < rows)
        spot = jnp.where(in_low, low_at, jnp.clip(high_at, 0, rows - 1) + rows)
        return spot, jnp.logical_or(in_low, in_high)

    def far_spot(row):
        away = row - mirror_far
        return jnp.clip(away, 0, rows - 1), jnp.logical_and(away >= 0, away < rows)

    def column_spot(row):
        away = row - (band - NY) * rows
        block = (away >= NY * rows).astype(jnp.int32) + (away >= 2 * NY * rows).astype(jnp.int32)
        within = away - block * (NY * rows)
        return block * rows + jnp.clip(within, 0, rows - 1), jnp.logical_and(within >= 0, within < rows)

    def taps(spot_of, t, r):
        first = itab[t, 0, r]
        out = []
        for a in range(4):
            spot, inside = spot_of(first + a)
            out.append((spot, jnp.where(inside, ftab[t, a, r], 0.0)))
        return out

    def weighted(ref, spots):
        acc = None
        for spot, weight in spots:
            term = weight * ref[spot]
            acc = term if acc is None else acc + term
        return acc

    def partial_rows(spot_of, src, jobs):
        def one(r, carry):
            for t, dst, extra in jobs:
                acc = weighted(src, taps(spot_of, t, r))
                dst[r] = acc if extra is None else acc + extra[r]
            return carry

        lax.fori_loop(0, rows, one, 0)

    def add_rows(n, dst, dst_at, extra):
        def one(r, carry):
            dst[dst_at + r] = dst[dst_at + r] + extra[r]
            return carry

        lax.fori_loop(0, n, one, 0)

    ready = []

    def need_tables():
        if ready:
            return
        ready.append(True)
        for copy in tables:
            copy.wait_recv()
        moves = [
            pltpu.make_async_copy(itab_all, itab, tab_local.at[0]),
            pltpu.make_async_copy(ftab_all, ftab, tab_local.at[1]),
        ]
        for copy in moves:
            copy.start()
        for copy in moves:
            copy.wait()

    half = rows // 2
    finals = [None] * count

    def stages_of(c):
        scheme = chunks[c][0]
        b = bufs[c]
        send = [bulk_send.at[c, k] for k in range(COPIES[scheme])]
        recv = [bulk_recv.at[c, k] for k in range(COPIES[scheme])]

        def link(k, src, dst, target):
            copy = remote(src, dst, send[k], recv[k], target)
            if target is up:
                return Guarded(copy, can_up, can_down)
            if target is down:
                return Guarded(copy, can_down, can_up)
            if target is toward:
                return Guarded(copy, to_down_up, to_up_down)
            if target is toward_main:
                return Guarded(copy, to_up_down, to_down_up)
            return copy

        if scheme == "ring":
            ring, send_up, send_down, recv_up, recv_down = b
            mine = ring.at[pl.ds(y * rows, rows)]
            from_down = ring.at[pl.ds(y_down * rows + half, rows - half)]
            from_up = ring.at[pl.ds(y_up * rows, half)]
            copies = [
                link(0, mine, mine, y_mates[0]), link(1, mine, mine, y_mates[2]),
                link(2, from_down, from_down, y_mates[0]), link(3, from_up, from_up, y_mates[2]),
                link(4, send_up, recv_up, up), link(5, send_down, recv_down, down),
            ]

            def stage0():
                copies[0].start()
                copies[1].start()

            def stage1():
                copies[0].wait_recv()
                copies[1].wait_recv()
                copies[2].start()
                copies[3].start()

            def stage2():
                copies[2].wait_recv()
                copies[3].wait_recv()
                need_tables()
                partial_rows(ring_spot, ring, [(1, send_up, None), (2, send_down, None)])
                copies[4].start()
                copies[5].start()

            def stage3():
                copies[4].wait_recv()
                copies[5].wait_recv()
                finals[c] = (ring_spot, ring, [recv_up, recv_down], None)

        elif scheme == "column":
            column, to_up, to_down, to_far, far_a, far_b, got_a, got_b = b
            mine = column.at[pl.ds(rows, rows)]
            copies = [
                link(0, mine, column.at[pl.ds(0, rows)], up), link(1, mine, column.at[pl.ds(2 * rows, rows)], down),
                link(2, to_far.at[pl.ds(0, half)], far_a, y_mates[0]),
                link(3, to_far.at[pl.ds(half, rows - half)], far_b, y_mates[2]),
                link(4, to_up, got_a, y_mates[0]), link(5, to_down, got_b, y_mates[2]),
            ]

            def stage0():
                copies[0].start()
                copies[1].start()

            def stage1():
                copies[0].wait_recv()
                copies[1].wait_recv()
                need_tables()
                partial_rows(column_spot, column, [(4, to_far, None)])
                copies[2].start()
                copies[3].start()
                partial_rows(column_spot, column, [(3, to_up, None), (5, to_down, None)])

            def stage2():
                copies[2].wait_recv()
                add_rows(half, to_up, 0, far_a)
                copies[4].start()
                copies[3].wait_recv()
                add_rows(rows - half, to_down, half, far_b)
                copies[5].start()

            def stage3():
                copies[4].wait_recv()
                copies[5].wait_recv()
                finals[c] = (column_spot, column, [got_a, got_b], None)

        elif scheme == "mirror":
            both, to_main, to_behind, to_far, to_cross, from_main, from_behind, passed, from_cross = b
            mine = both.at[pl.ds(south * rows, rows)]
            copies = [
                link(0, mine, mine, cross), link(1, to_main, from_main, toward_main),
                link(2, to_behind, from_behind, behind), link(3, to_far, passed, toward_main),
                link(4, to_cross, from_cross, pair),
            ]
            raw = link(2, mine, from_behind, behind)

            def stage0():
                copies[0].start()
                pl.when(outer)(lambda: raw.start())

            def stage1():
                copies[0].wait_recv()
                need_tables()
                partial_rows(mirror_spot, both, [(7, to_far, None)])
                copies[3].start()
                partial_rows(mirror_spot, both, [(1 + south, to_main, None)])
                copies[1].start()

                @pl.when(inner)
                def _():
                    partial_rows(mirror_spot, both, [(2 - south, to_behind, None)])
                    copies[2].start()

            def stage2():
                copies[3].wait_recv()
                partial_rows(mirror_spot, both, [(3 + 2 * odd, to_cross, passed)])

                @pl.when(outer)
                def _():
                    copies[2].wait_recv()

                    def one(r, carry):
                        to_cross[r] = to_cross[r] + weighted(from_behind, taps(far_spot, 3 + 2 * odd, r))
                        return carry

                    lax.fori_loop(0, rows, one, 0)

                copies[4].start()

            def stage3():
                copies[1].wait_recv()
                copies[4].wait_recv()
                pl.when(inner)(lambda: copies[2].wait_recv())
                finals[c] = (mirror_spot, both, [from_main, from_cross], from_behind)

        else:
            both, to_up, to_down, to_diag, to_cross, from_down, from_up, passed, from_cross = b
            mine = both.at[pl.ds(odd * rows, rows)]
            copies = [
                link(0, mine, mine, pair), link(1, to_up, from_down, up), link(2, to_down, from_up, down),
                link(3, to_diag, passed, toward), link(4, to_cross, from_cross, cross),
            ]

            def stage0():
                copies[0].start()

            def stage1():
                copies[0].wait_recv()
                need_tables()
                partial_rows(pair_spot, both, [(6, to_diag, None)])
                copies[3].start()
                partial_rows(pair_spot, both, [(1, to_up, None), (2, to_down, None)])
                copies[1].start()
                copies[2].start()

            def stage2():
                copies[3].wait_recv()
                partial_rows(pair_spot, both, [(5 - 2 * odd, to_cross, passed)])
                copies[4].start()

            def stage3():
                copies[1].wait_recv()
                copies[2].wait_recv()
                copies[4].wait_recv()
                finals[c] = (pair_spot, both, [from_down, from_up, from_cross], None)

        return copies, [stage0, stage1, stage2, stage3]

    phases = [y_mates, z_mates, c_mates, x_mates]
    offsets = [0]
    for mates in phases:
        offsets.append(offsets[-1] + len(mates))
    mass_copies = []
    for k, mates in enumerate(phases):
        mass_copies.append([
            remote(mass.at[k], mass.at[len(phases) + offsets[k] + i], mass_send.at[offsets[k] + i],
                   mass_recv.at[offsets[k] + i], mate)
            for i, mate in enumerate(mates)
        ])

    def mass_step(step):
        if step == 0:
            need_tables()
            for copy in sum_copies:
                copy.wait_recv()

            def one(r, carry):
                before, after = carry
                before = before + ftab[0, 9, r] * sums[y * rows + r]
                for t in range(3):
                    after = after + ftab[t, 4, r] * weighted(sums, taps(ring_spot, t, r))
                return before, after

            zero = jnp.zeros((8, LANES), jnp.float32)
            before, after = lax.fori_loop(0, rows, one, (zero, zero))
            total = jnp.concatenate([before[0:4], after[0:4]], axis=0)
        else:
            k = step - 1
            total = mass[k]
            for i, copy in enumerate(mass_copies[k]):
                copy.wait_recv()
                total = total + mass[len(phases) + offsets[k] + i]
        if step < len(phases):
            mass[step] = total
            for copy in mass_copies[step]:
                copy.start()
        else:
            total = jnp.sum(total, axis=1, keepdims=True)
            ratio_ref[0:4] = jnp.broadcast_to(total[0:4] / total[4:8], (4, LANES))


    def finish(c):
        _, f, lane, width = chunks[c]
        spot_of, src, extras, far = finals[c]

        def one(r, carry):
            acc = weighted(src, taps(spot_of, 0, r))
            for extra in extras:
                acc = acc + extra[r]
            out_ref[r, f, :, lane:lane + width] = acc
            return carry

        lax.fori_loop(0, rows, one, 0)
        if far is None:
            return

        @pl.when(inner)
        def _():
            def more(r, carry):
                out_ref[r, f, :, lane:lane + width] = out_ref[r, f, :, lane:lane + width] + far[r]
                return carry

            lax.fori_loop(0, rows, more, 0)

        @pl.when(outer)
        def _():
            def more(r, carry):
                acc = weighted(far, taps(far_spot, 0, r))
                out_ref[r, f, :, lane:lane + width] = out_ref[r, f, :, lane:lane + width] + acc
                return carry

            lax.fori_loop(0, rows, more, 0)

    def filter_rows(f):
        def one(i, carry):
            for r in (2 * i, 2 * i + 1):
                column = out_ref[r, f]
                mixed = ftab[0, 5, r] * column
                for k in range(1, 4):
                    mixed = mixed + ftab[0, 5 + k, r] * pltpu.roll(column, lon - k, 1)
                out_ref[r, f] = mixed
            return carry

        lax.fori_loop(0, rows // 2, one, 0)

    every = [stages_of(c) for c in range(count)]
    place = [0] * count
    left = [sum(1 for chunk in chunks if chunk[1] == f) for f in range(nfields)]
    mass_done = 0
    for i, c in enumerate(ORDER):
        every[c][1][place[c]]()
        place[c] += 1
        if place[c] == 4:
            finish(c)
            f = chunks[c][1]
            left[f] -= 1
            if left[f] == 0:
                filter_rows(f)
        while mass_done < len(MASS_AT) and MASS_AT[mass_done] == i:
            mass_step(mass_done)
            mass_done += 1

    for copies, _ in every:
        for copy in copies:
            copy.wait_send()
    for copy in tables + sum_copies:
        copy.wait_send()
    for group in mass_copies:
        for copy in group:
            copy.wait_send()


def turn_kernel(nfields, lon, shift_ref, ratio_ref, column_ref, out_ref):
    lane_id = lax.broadcasted_iota(jnp.int32, (8, LANES), 1)
    tiles = lon // LANES
    for i in range(ROWS_PER_STEP):
        r = pl.program_id(0) * ROWS_PER_STEP + i
        begin = shift_ref[r] - 1
        begin = jnp.where(begin < 0, begin + lon, begin)
        whole = lax.shift_right_logical(begin, 7)
        rest = jnp.bitwise_and(begin, LANES - 1)
        turn = jnp.bitwise_and(LANES - rest, LANES - 1)
        keep = lane_id < (LANES - rest)
        spots = []
        for t in range(tiles + 1):
            spot = whole + t
            spot = jnp.where(spot >= tiles, spot - tiles, spot)
            spots.append(pl.multiple_of(spot * LANES, LANES))
        for f in range(nfields):
            ratio = jnp.broadcast_to(ratio_ref[f:f + 1, :], (8, LANES))
            turned = [pltpu.roll(column_ref[r, f, :, pl.ds(spot, LANES)], turn, 1) for spot in spots]
            for t in range(tiles):
                out_ref[i, f, :, t * LANES:(t + 1) * LANES] = jnp.where(keep, turned[t], turned[t + 1]) * ratio


def per_device(fields, lat_fraction, lon_fraction, lon_shift, departure_row, extents):
    rows, nfields, levels, lon = fields.shape
    chunks = [(k, f, lane * LANES, width * LANES) for k, f, lane, width in CHUNKS]
    count = len(chunks)
    dma = pltpu.SemaphoreType.DMA
    mates = (NX - 1) + 1 + (NZ - 1) + (NY - 1)
    scratch = []
    for scheme, _, _, width in chunks:
        scratch += buffers_of(scheme, rows, levels, width)
    scratch += [
        pltpu.VMEM((NY * rows, 8, LANES), jnp.float32),
        pltpu.VMEM((8, 8, LANES), jnp.int32),
        pltpu.VMEM((8, 16, LANES), jnp.float32),
        pltpu.SMEM((8, 8, LANES), jnp.int32),
        pltpu.SMEM((8, 16, LANES), jnp.float32),
        pltpu.VMEM((4 + mates, 8, LANES), jnp.float32),
        dma((count,)), dma((count, 6)), dma((count, 6)), dma((14,)), dma((14,)), dma((2,)),
        dma((NY - 1,)), dma((NY - 1,)), dma((mates,)), dma((mates,)), dma((nfields,)),
    ]
    vmem = pl.BlockSpec(memory_space=pltpu.VMEM)
    column, ratio = pl.pallas_call(
        functools.partial(advect_kernel, rows, nfields, lon, chunks),
        out_shape=(
            jax.ShapeDtypeStruct(fields.shape, fields.dtype),
            jax.ShapeDtypeStruct((4, LANES), jnp.float32),
        ),
        in_specs=[vmem, vmem, pl.BlockSpec(memory_space=pl.ANY)],
        out_specs=(vmem, vmem),
        scratch_shapes=scratch,
        compiler_params=pltpu.CompilerParams(collective_id=0, has_side_effects=True, vmem_limit_bytes=KERNEL_VMEM),
    )(jnp.stack([lat_fraction, lon_fraction]), jnp.concatenate([departure_row[None], extents], axis=1), fields)
    block = pl.BlockSpec((ROWS_PER_STEP, nfields, levels, lon), lambda i: (i, 0, 0, 0))
    return pl.pallas_call(
        functools.partial(turn_kernel, nfields, lon),
        grid=(rows // ROWS_PER_STEP,),
        out_shape=jax.ShapeDtypeStruct(fields.shape, fields.dtype),
        in_specs=[pl.BlockSpec(memory_space=pltpu.SMEM), vmem, vmem],
        out_specs=block,
        compiler_params=pltpu.CompilerParams(vmem_limit_bytes=16 * 1024 * 1024),
    )(lon_shift, ratio, column)


def solution(mesh):
    placed = (P("lat", None, "lev", None), P("lat"), P("lat"), P("lat"), P("lat"), P("lat", None))
    return jax.shard_map(
        per_device,
        mesh=mesh,
        in_specs=placed,
        out_specs=P("lat", None, "lev", None),
        check_vma=False,
    )
```

```python
import functools
import math

import jax
import jax.numpy as jnp
from jax import lax
from jax.experimental import pallas as pl
from jax.experimental.pallas import tpu as pltpu
from jax.sharding import PartitionSpec as P

MESH = pl.DeviceIdType.MESH
NY, NZ, NX = 4, 8, 4
LANES = 128
ROWS_PER_STEP = 5
UNROLL = 2
KERNEL_VMEM = 50 * 1024 * 1024
CHUNKS = [('column', 0, 0, 10), ('mirror', 0, 10, 10), ('ring', 1, 0, 15), ('column', 1, 15, 5), ('mirror', 2, 0, 5), ('pair', 2, 5, 15)]
ORDER = [0, 4, 5, 1, 2, 3, 4, 0, 5, 1, 2, 0, 3, 5, 1, 2, 0, 4, 3, 1, 4, 5, 2, 3]
MASS_AT = [2, 8, 18, 18, 23]


def cubic_weights(fraction):
    return [
        -fraction * (fraction - 1.0) * (fraction - 2.0) / 6.0,
        (fraction + 1.0) * (fraction - 1.0) * (fraction - 2.0) / 2.0,
        -(fraction + 1.0) * fraction * (fraction - 2.0) / 2.0,
        (fraction + 1.0) * fraction * (fraction - 1.0) / 6.0,
    ]


def buffers_of(scheme, rows, levels, width):
    half = rows // 2
    counts = {
        "ring": [NY * rows] + [rows] * 4,
        "column": [3 * rows] + [rows] * 3 + [half, rows - half] + [rows] * 2,
        "pair": [2 * rows] + [rows] * 8,
        "mirror": [2 * rows] + [rows] * 8,
    }[scheme]
    return [pltpu.VMEM((n, levels, width), jnp.float32) for n in counts]


COPIES = {"ring": 6, "column": 6, "pair": 5, "mirror": 5}


class Guarded:
    def __init__(self, copy, sends, gets):
        self.copy, self.sends, self.gets = copy, sends, gets

    def start(self):
        pl.when(self.sends)(lambda: self.copy.start())

    def wait_recv(self):
        pl.when(self.gets)(lambda: self.copy.wait_recv())

    def wait_send(self):
        pl.when(self.sends)(lambda: self.copy.wait_send())


def advect_kernel(rows, nfields, lon, chunks, *refs):
    refs = list(refs)
    fractions_ref, numbers_ref, fields_ref, out_ref, ratio_ref = refs[:5]
    scratch = refs[5:]
    count = len(chunks)
    bufs = []
    for chunk in chunks:
        n = len(buffers_of(chunk[0], rows, 8, LANES))
        bufs.append(scratch[:n])
        scratch = scratch[n:]
    (sums, itab_all, ftab_all, itab, ftab, mass,
     load_sem, bulk_send, bulk_recv, tab_send, tab_recv, tab_local,
     sum_send, sum_recv, mass_send, mass_recv, out_sem) = scratch

    band = lax.axis_index("lat")
    core = lax.axis_index("lev")
    bands = NX * NZ * NY
    y = lax.rem(band, NY)
    z = lax.rem(lax.div(band, NY), NZ)
    x = lax.div(band, NY * NZ)
    base = band - y
    odd = lax.rem(y, 2)
    south = lax.div(y, 2)

    y_up, y_down = lax.rem(y + 1, NY), lax.rem(y + 3, NY)
    y_mates = [(base + lax.rem(y + s, NY), core) for s in (1, 2, 3)]
    z_mates = [(x * (NY * NZ) + lax.rem(z + s, NZ) * NY + y, core) for s in range(1, NZ)]
    x_mates = [(lax.rem(x + s, NX) * (NY * NZ) + z * NY + y, core) for s in range(1, NX)]
    c_mates = [(band, 1 - core)]
    up = (lax.rem(band + NY, bands), core)
    down = (lax.rem(band + bands - NY, bands), core)
    pair = (band + 1 - 2 * odd, core)
    cross = (base + 3 - y, core)
    toward = (lax.rem(band + bands - NY + 2 * NY * south, bands), core)
    diagonal = (lax.rem(base + 3 - y + bands - NY + 2 * NY * south, bands), core)
    outer = jnp.logical_or(y == 0, y == NY - 1)
    inner = jnp.logical_not(outer)
    toward_main = (lax.rem(band + NY + bands - 2 * NY * south, bands), core)
    behind = toward
    before = (lax.rem(band + 1 - 2 * odd + NY + bands - 2 * NY * south, bands), core)
    after = (lax.rem(band + 1 - 2 * odd + bands - NY + 2 * NY * south, bands), core)
    partners = y_mates + z_mates + x_mates + c_mates + [up, down, diagonal, before, after]

    own_at = {"ring": y * rows, "column": rows, "pair": odd * rows, "mirror": south * rows}
    loads = [
        pltpu.make_async_copy(
            fields_ref.at[:, f, :, pl.ds(lane, width)],
            bufs[c][0].at[pl.ds(own_at[scheme], rows)],
            load_sem.at[c],
        )
        for c, (scheme, f, lane, width) in enumerate(chunks)
    ]
    loaded_first = []
    for c in ORDER + list(range(count)):
        if c not in loaded_first:
            loaded_first.append(c)
    for c in loaded_first:
        loads[c].start()

    can_up, can_down = band + NY < bands, band >= NY
    by_half = lambda north, south_side: jnp.logical_or(
        jnp.logical_and(south == 0, north), jnp.logical_and(south == 1, south_side)
    )
    to_up_down, to_down_up = by_half(can_up, can_down), by_half(can_down, can_up)

    barrier = pltpu.get_barrier_semaphore()
    for partner in partners:
        pl.semaphore_signal(barrier, inc=1, device_id=partner, device_id_type=MESH)

    def clear(ref, first, n):
        def one(r, carry):
            ref[first + r] = jnp.zeros(ref.shape[1:], jnp.float32)
            return carry

        lax.fori_loop(0, n, one, 0)

    for at_end, side in ((jnp.logical_not(can_down), 0), (jnp.logical_not(can_up), 1)):

        @pl.when(at_end)
        def _(side=side):
            for b, chunk in zip(bufs, chunks):
                if chunk[0] == "ring":
                    clear(b[3 + side], 0, rows)
                elif chunk[0] == "column":
                    clear(b[0], 2 * side * rows, rows)
                elif chunk[0] == "pair":
                    clear(b[5 + side], 0, rows)
                    pl.when(south == 1 - side)(lambda b=b: clear(b[7], 0, rows))
                else:
                    pl.when(south == side)(lambda b=b: clear(b[5], 0, rows))
                    pl.when(south == side)(lambda b=b: clear(b[7], 0, rows))
                    pl.when(south == 1 - side)(lambda b=b: clear(b[6], 0, rows))

    first_row = band * rows
    low = first_row - numbers_ref[0:1, rows:rows + 1] * rows + 1
    high = first_row + rows - 3 + numbers_ref[0:1, rows + 1:rows + 2] * rows
    start = jnp.minimum(jnp.maximum(numbers_ref[0:1, 0:rows], low), high)
    start = jnp.minimum(jnp.maximum(start, 1), bands * rows - 3) - 1
    lat_w = cubic_weights(fractions_ref[0:1])
    lon_w = cubic_weights(fractions_ref[1:2])
    row_ids = first_row + lax.broadcasted_iota(jnp.int32, (1, rows), 1)
    area = jnp.cos(math.pi * (row_ids.astype(jnp.float32) + 0.5) / (bands * rows) - math.pi / 2.0)
    lon_total = lon_w[0] + lon_w[1] + lon_w[2] + lon_w[3]
    itab_all[0] = jnp.zeros((8, LANES), jnp.int32)
    ftab_all[0] = jnp.zeros((16, LANES), jnp.float32)
    itab_all[0, 0:1, 0:rows] = start
    for k, values in enumerate(lat_w + [area * lon_total] + lon_w + [area]):
        ftab_all[0, k:k + 1, 0:rows] = values

    for load in loads:
        load.wait()

    def row_sums(r, carry):
        pieces = []
        for f in range(nfields):
            total = None
            for c, (scheme, field, lane, width) in enumerate(chunks):
                if field != f:
                    continue
                block = bufs[c][0][own_at[scheme] + r]
                for t in range(width // LANES):
                    tile = block[:, t * LANES:(t + 1) * LANES]
                    total = tile if total is None else total + tile
            pieces.append(jnp.sum(total, axis=0, keepdims=True))
        pieces.append(jnp.zeros((8 - nfields, LANES), jnp.float32))
        sums[y * rows + r] = jnp.concatenate(pieces, axis=0)
        return carry

    lax.fori_loop(0, rows, row_sums, 0)
    pl.semaphore_wait(barrier, len(partners))

    def remote(src, dst, send_sem, recv_sem, target):
        return pltpu.make_async_remote_copy(
            src_ref=src, dst_ref=dst, send_sem=send_sem, recv_sem=recv_sem, device_id=target, device_id_type=MESH
        )

    table_routes = [(2, up), (1, down), (5, y_mates[0]), (4, y_mates[1]), (3, y_mates[2]), (6, diagonal), (7, after)]
    tables = []
    for i, (slot, target) in enumerate(table_routes):
        for j, ref in enumerate((itab_all, ftab_all)):
            tables.append(remote(ref.at[0], ref.at[slot], tab_send.at[2 * i + j], tab_recv.at[2 * i + j], target))
    for copy in tables:
        copy.start()
    my_sums = sums.at[pl.ds(y * rows, rows)]
    sum_copies = [remote(my_sums, my_sums, sum_send.at[s], sum_recv.at[s], y_mates[s]) for s in range(NY - 1)]
    for copy in sum_copies:
        copy.start()

    def ring_spot(row):
        spot = row - base * rows
        return jnp.clip(spot, 0, NY * rows - 1), jnp.logical_and(spot >= 0, spot < NY * rows)

    def pair_spot(row):
        spot = row - (band - odd) * rows
        return jnp.clip(spot, 0, 2 * rows - 1), jnp.logical_and(spot >= 0, spot < 2 * rows)

    mirror_low = (base + jnp.where(outer, 0, 1)) * rows
    mirror_high = (base + jnp.where(outer, 3, 2)) * rows
    mirror_far = (band + NY - 2 * NY * south) * rows

    def mirror_spot(row):
        low_at, high_at = row - mirror_low, row - mirror_high
        in_low = jnp.logical_and(low_at >= 0, low_at < rows)
        in_high = jnp.logical_and(high_at >= 0, high_at < rows)
        spot = jnp.where(in_low, low_at, jnp.clip(high_at, 0, rows - 1) + rows)
        return spot, jnp.logical_or(in_low, in_high)

    def far_spot(row):
        away = row - mirror_far
        return jnp.clip(away, 0, rows - 1), jnp.logical_and(away >= 0, away < rows)

    def column_spot(row):
        away = row - (band - NY) * rows
        block = (away >= NY * rows).astype(jnp.int32) + (away >= 2 * NY * rows).astype(jnp.int32)
        within = away - block * (NY * rows)
        return block * rows + jnp.clip(within, 0, rows - 1), jnp.logical_and(within >= 0, within < rows)

    def taps(spot_of, t, r):
        first = itab[t, 0, r]
        out = []
        for a in range(4):
            spot, inside = spot_of(first + a)
            out.append((spot, jnp.where(inside, ftab[t, a, r], 0.0)))
        return out

    def weighted(ref, spots):
        acc = None
        for spot, weight in spots:
            term = weight * ref[spot]
            acc = term if acc is None else acc + term
        return acc

    def each_row(one):
        def several(i, carry):
            for k in range(UNROLL):
                one(UNROLL * i + k)
            return carry

        lax.fori_loop(0, rows // UNROLL, several, 0)

    def partial_rows(spot_of, src, jobs):
        def one(r):
            for t, dst, extra in jobs:
                acc = weighted(src, taps(spot_of, t, r))
                dst[r] = acc if extra is None else acc + extra[r]

        each_row(one)

    def add_rows(n, dst, dst_at, extra):
        def one(r, carry):
            dst[dst_at + r] = dst[dst_at + r] + extra[r]
            return carry

        lax.fori_loop(0, n, one, 0)

    ready = []

    def need_tables():
        if ready:
            return
        ready.append(True)
        for copy in tables:
            copy.wait_recv()
        moves = [
            pltpu.make_async_copy(itab_all, itab, tab_local.at[0]),
            pltpu.make_async_copy(ftab_all, ftab, tab_local.at[1]),
        ]
        for copy in moves:
            copy.start()
        for copy in moves:
            copy.wait()

    half = rows // 2
    finals = [None] * count

    def stages_of(c):
        scheme = chunks[c][0]
        b = bufs[c]
        send = [bulk_send.at[c, k] for k in range(COPIES[scheme])]
        recv = [bulk_recv.at[c, k] for k in range(COPIES[scheme])]

        def link(k, src, dst, target):
            copy = remote(src, dst, send[k], recv[k], target)
            if target is up:
                return Guarded(copy, can_up, can_down)
            if target is down:
                return Guarded(copy, can_down, can_up)
            if target is toward:
                return Guarded(copy, to_down_up, to_up_down)
            if target is toward_main:
                return Guarded(copy, to_up_down, to_down_up)
            return copy

        if scheme == "ring":
            ring, send_up, send_down, recv_up, recv_down = b
            mine = ring.at[pl.ds(y * rows, rows)]
            from_down = ring.at[pl.ds(y_down * rows + half, rows - half)]
            from_up = ring.at[pl.ds(y_up * rows, half)]
            copies = [
                link(0, mine, mine, y_mates[0]), link(1, mine, mine, y_mates[2]),
                link(2, from_down, from_down, y_mates[0]), link(3, from_up, from_up, y_mates[2]),
                link(4, send_up, recv_up, up), link(5, send_down, recv_down, down),
            ]

            def stage0():
                copies[0].start()
                copies[1].start()

            def stage1():
                copies[0].wait_recv()
                copies[1].wait_recv()
                copies[2].start()
                copies[3].start()

            def stage2():
                copies[2].wait_recv()
                copies[3].wait_recv()
                need_tables()
                partial_rows(ring_spot, ring, [(1, send_up, None), (2, send_down, None)])
                copies[4].start()
                copies[5].start()

            def stage3():
                copies[4].wait_recv()
                copies[5].wait_recv()
                finals[c] = (ring_spot, ring, [recv_up, recv_down], None)

        elif scheme == "column":
            column, to_up, to_down, to_far, far_a, far_b, got_a, got_b = b
            mine = column.at[pl.ds(rows, rows)]
            copies = [
                link(0, mine, column.at[pl.ds(0, rows)], up), link(1, mine, column.at[pl.ds(2 * rows, rows)], down),
                link(2, to_far.at[pl.ds(0, half)], far_a, y_mates[0]),
                link(3, to_far.at[pl.ds(half, rows - half)], far_b, y_mates[2]),
                link(4, to_up, got_a, y_mates[0]), link(5, to_down, got_b, y_mates[2]),
            ]

            def stage0():
                copies[0].start()
                copies[1].start()

            def stage1():
                copies[0].wait_recv()
                copies[1].wait_recv()
                need_tables()
                partial_rows(column_spot, column, [(4, to_far, None)])
                copies[2].start()
                copies[3].start()
                partial_rows(column_spot, column, [(3, to_up, None), (5, to_down, None)])

            def stage2():
                copies[2].wait_recv()
                add_rows(half, to_up, 0, far_a)
                copies[4].start()
                copies[3].wait_recv()
                add_rows(rows - half, to_down, half, far_b)
                copies[5].start()

            def stage3():
                copies[4].wait_recv()
                copies[5].wait_recv()
                finals[c] = (column_spot, column, [got_a, got_b], None)

        elif scheme == "mirror":
            both, to_main, to_behind, to_far, to_cross, from_main, from_behind, passed, from_cross = b
            mine = both.at[pl.ds(south * rows, rows)]
            copies = [
                link(0, mine, mine, cross), link(1, to_main, from_main, toward_main),
                link(2, to_behind, from_behind, behind), link(3, to_far, passed, toward_main),
                link(4, to_cross, from_cross, pair),
            ]
            raw = link(2, mine, from_behind, behind)

            def stage0():
                copies[0].start()
                pl.when(outer)(lambda: raw.start())

            def stage1():
                copies[0].wait_recv()
                need_tables()
                partial_rows(mirror_spot, both, [(7, to_far, None)])
                copies[3].start()
                partial_rows(mirror_spot, both, [(1 + south, to_main, None)])
                copies[1].start()

                @pl.when(inner)
                def _():
                    partial_rows(mirror_spot, both, [(2 - south, to_behind, None)])
                    copies[2].start()

            def stage2():
                copies[3].wait_recv()
                partial_rows(mirror_spot, both, [(3 + 2 * odd, to_cross, passed)])

                @pl.when(outer)
                def _():
                    copies[2].wait_recv()

                    def one(r, carry):
                        to_cross[r] = to_cross[r] + weighted(from_behind, taps(far_spot, 3 + 2 * odd, r))
                        return carry

                    lax.fori_loop(0, rows, one, 0)

                copies[4].start()

            def stage3():
                copies[1].wait_recv()
                copies[4].wait_recv()
                pl.when(inner)(lambda: copies[2].wait_recv())
                finals[c] = (mirror_spot, both, [from_main, from_cross], from_behind)

        else:
            both, to_up, to_down, to_diag, to_cross, from_down, from_up, passed, from_cross = b
            mine = both.at[pl.ds(odd * rows, rows)]
            copies = [
                link(0, mine, mine, pair), link(1, to_up, from_down, up), link(2, to_down, from_up, down),
                link(3, to_diag, passed, toward), link(4, to_cross, from_cross, cross),
            ]

            def stage0():
                copies[0].start()

            def stage1():
                copies[0].wait_recv()
                need_tables()
                partial_rows(pair_spot, both, [(6, to_diag, None)])
                copies[3].start()
                partial_rows(pair_spot, both, [(1, to_up, None), (2, to_down, None)])
                copies[1].start()
                copies[2].start()

            def stage2():
                copies[3].wait_recv()
                partial_rows(pair_spot, both, [(5 - 2 * odd, to_cross, passed)])
                copies[4].start()

            def stage3():
                copies[1].wait_recv()
                copies[2].wait_recv()
                copies[4].wait_recv()
                finals[c] = (pair_spot, both, [from_down, from_up, from_cross], None)

        return copies, [stage0, stage1, stage2, stage3]

    phases = [y_mates, z_mates, c_mates, x_mates]
    offsets = [0]
    for mates in phases:
        offsets.append(offsets[-1] + len(mates))
    mass_copies = []
    for k, mates in enumerate(phases):
        mass_copies.append([
            remote(mass.at[k], mass.at[len(phases) + offsets[k] + i], mass_send.at[offsets[k] + i],
                   mass_recv.at[offsets[k] + i], mate)
            for i, mate in enumerate(mates)
        ])

    def mass_step(step):
        if step == 0:
            need_tables()
            for copy in sum_copies:
                copy.wait_recv()

            def one(r, carry):
                before, after = carry
                before = before + ftab[0, 9, r] * sums[y * rows + r]
                for t in range(3):
                    after = after + ftab[t, 4, r] * weighted(sums, taps(ring_spot, t, r))
                return before, after

            zero = jnp.zeros((8, LANES), jnp.float32)
            before, after = lax.fori_loop(0, rows, one, (zero, zero))
            total = jnp.concatenate([before[0:4], after[0:4]], axis=0)
        else:
            k = step - 1
            total = mass[k]
            for i, copy in enumerate(mass_copies[k]):
                copy.wait_recv()
                total = total + mass[len(phases) + offsets[k] + i]
        if step < len(phases):
            mass[step] = total
            for copy in mass_copies[step]:
                copy.start()
        else:
            total = jnp.sum(total, axis=1, keepdims=True)
            ratio_ref[0:4] = jnp.broadcast_to(total[0:4] / total[4:8], (4, LANES))


    def finish(c):
        _, f, lane, width = chunks[c]
        spot_of, src, extras, far = finals[c]

        def one(r):
            acc = weighted(src, taps(spot_of, 0, r))
            for extra in extras:
                acc = acc + extra[r]
            out_ref[r, f, :, lane:lane + width] = acc

        each_row(one)
        if far is None:
            return

        @pl.when(inner)
        def _():
            def more(r, carry):
                out_ref[r, f, :, lane:lane + width] = out_ref[r, f, :, lane:lane + width] + far[r]
                return carry

            lax.fori_loop(0, rows, more, 0)

        @pl.when(outer)
        def _():
            def more(r, carry):
                acc = weighted(far, taps(far_spot, 0, r))
                out_ref[r, f, :, lane:lane + width] = out_ref[r, f, :, lane:lane + width] + acc
                return carry

            lax.fori_loop(0, rows, more, 0)

    def filter_rows(f):
        def one(r):
            column = out_ref[r, f]
            mixed = ftab[0, 5, r] * column
            for k in range(1, 4):
                mixed = mixed + ftab[0, 5 + k, r] * pltpu.roll(column, lon - k, 1)
            out_ref[r, f] = mixed

        each_row(one)

    every = [stages_of(c) for c in range(count)]
    place = [0] * count
    left = [sum(1 for chunk in chunks if chunk[1] == f) for f in range(nfields)]
    mass_done = 0
    for i, c in enumerate(ORDER):
        every[c][1][place[c]]()
        place[c] += 1
        if place[c] == 4:
            finish(c)
            f = chunks[c][1]
            left[f] -= 1
            if left[f] == 0:
                filter_rows(f)
        while mass_done < len(MASS_AT) and MASS_AT[mass_done] == i:
            mass_step(mass_done)
            mass_done += 1

    for copies, _ in every:
        for copy in copies:
            copy.wait_send()
    for copy in tables + sum_copies:
        copy.wait_send()
    for group in mass_copies:
        for copy in group:
            copy.wait_send()


def turn_kernel(nfields, lon, shift_ref, ratio_ref, column_ref, out_ref):
    lane_id = lax.broadcasted_iota(jnp.int32, (8, LANES), 1)
    tiles = lon // LANES
    for i in range(ROWS_PER_STEP):
        r = pl.program_id(0) * ROWS_PER_STEP + i
        begin = shift_ref[r] - 1
        begin = jnp.where(begin < 0, begin + lon, begin)
        whole = lax.shift_right_logical(begin, 7)
        rest = jnp.bitwise_and(begin, LANES - 1)
        turn = jnp.bitwise_and(LANES - rest, LANES - 1)
        keep = lane_id < (LANES - rest)
        spots = []
        for t in range(tiles + 1):
            spot = whole + t
            spot = jnp.where(spot >= tiles, spot - tiles, spot)
            spots.append(pl.multiple_of(spot * LANES, LANES))
        for f in range(nfields):
            ratio = jnp.broadcast_to(ratio_ref[f:f + 1, :], (8, LANES))
            turned = [pltpu.roll(column_ref[r, f, :, pl.ds(spot, LANES)], turn, 1) for spot in spots]
            for t in range(tiles):
                out_ref[i, f, :, t * LANES:(t + 1) * LANES] = jnp.where(keep, turned[t], turned[t + 1]) * ratio


def per_device(fields, lat_fraction, lon_fraction, lon_shift, departure_row, extents):
    rows, nfields, levels, lon = fields.shape
    chunks = [(k, f, lane * LANES, width * LANES) for k, f, lane, width in CHUNKS]
    count = len(chunks)
    dma = pltpu.SemaphoreType.DMA
    mates = (NX - 1) + 1 + (NZ - 1) + (NY - 1)
    scratch = []
    for scheme, _, _, width in chunks:
        scratch += buffers_of(scheme, rows, levels, width)
    scratch += [
        pltpu.VMEM((NY * rows, 8, LANES), jnp.float32),
        pltpu.VMEM((8, 8, LANES), jnp.int32),
        pltpu.VMEM((8, 16, LANES), jnp.float32),
        pltpu.SMEM((8, 8, LANES), jnp.int32),
        pltpu.SMEM((8, 16, LANES), jnp.float32),
        pltpu.VMEM((4 + mates, 8, LANES), jnp.float32),
        dma((count,)), dma((count, 6)), dma((count, 6)), dma((14,)), dma((14,)), dma((2,)),
        dma((NY - 1,)), dma((NY - 1,)), dma((mates,)), dma((mates,)), dma((nfields,)),
    ]
    vmem = pl.BlockSpec(memory_space=pltpu.VMEM)
    column, ratio = pl.pallas_call(
        functools.partial(advect_kernel, rows, nfields, lon, chunks),
        out_shape=(
            jax.ShapeDtypeStruct(fields.shape, fields.dtype),
            jax.ShapeDtypeStruct((4, LANES), jnp.float32),
        ),
        in_specs=[vmem, vmem, pl.BlockSpec(memory_space=pl.ANY)],
        out_specs=(vmem, vmem),
        scratch_shapes=scratch,
        compiler_params=pltpu.CompilerParams(collective_id=0, has_side_effects=True, vmem_limit_bytes=KERNEL_VMEM),
    )(jnp.stack([lat_fraction, lon_fraction]), jnp.concatenate([departure_row[None], extents], axis=1), fields)
    block = pl.BlockSpec((ROWS_PER_STEP, nfields, levels, lon), lambda i: (i, 0, 0, 0))
    return pl.pallas_call(
        functools.partial(turn_kernel, nfields, lon),
        grid=(rows // ROWS_PER_STEP,),
        out_shape=jax.ShapeDtypeStruct(fields.shape, fields.dtype),
        in_specs=[pl.BlockSpec(memory_space=pltpu.SMEM), vmem, vmem],
        out_specs=block,
        compiler_params=pltpu.CompilerParams(vmem_limit_bytes=16 * 1024 * 1024),
    )(lon_shift, ratio, column)


def solution(mesh):
    placed = (P("lat", None, "lev", None), P("lat"), P("lat"), P("lat"), P("lat"), P("lat", None))
    return jax.shard_map(
        per_device,
        mesh=mesh,
        in_specs=placed,
        out_specs=P("lat", None, "lev", None),
        check_vma=False,
    )
```

```python
import functools
import math

import jax
import jax.numpy as jnp
from jax import lax
from jax.experimental import pallas as pl
from jax.experimental.pallas import tpu as pltpu
from jax.sharding import PartitionSpec as P

MESH = pl.DeviceIdType.MESH
NY, NZ, NX = 4, 8, 4
LANES = 128
ROWS_PER_STEP = 1
UNROLL = 2
KERNEL_VMEM = 50 * 1024 * 1024
CHUNKS = [('column', 0, 0, 10), ('mirror', 0, 10, 10), ('ring', 1, 0, 15), ('column', 1, 15, 5), ('mirror', 2, 0, 5), ('pair', 2, 5, 15)]
ORDER = [0, 4, 5, 1, 2, 3, 4, 0, 5, 1, 2, 0, 3, 5, 1, 2, 0, 4, 3, 1, 4, 5, 2, 3]
MASS_AT = [2, 8, 18, 18, 23]


def cubic_weights(fraction):
    return [
        -fraction * (fraction - 1.0) * (fraction - 2.0) / 6.0,
        (fraction + 1.0) * (fraction - 1.0) * (fraction - 2.0) / 2.0,
        -(fraction + 1.0) * fraction * (fraction - 2.0) / 2.0,
        (fraction + 1.0) * fraction * (fraction - 1.0) / 6.0,
    ]


def buffers_of(scheme, rows, levels, width):
    half = rows // 2
    counts = {
        "ring": [NY * rows] + [rows] * 4,
        "column": [3 * rows] + [rows] * 3 + [half, rows - half] + [rows] * 2,
        "pair": [2 * rows] + [rows] * 8,
        "mirror": [2 * rows] + [rows] * 8,
    }[scheme]
    return [pltpu.VMEM((n, levels, width), jnp.float32) for n in counts]


COPIES = {"ring": 6, "column": 6, "pair": 5, "mirror": 5}


class Guarded:
    def __init__(self, copy, sends, gets):
        self.copy, self.sends, self.gets = copy, sends, gets

    def start(self):
        pl.when(self.sends)(lambda: self.copy.start())

    def wait_recv(self):
        pl.when(self.gets)(lambda: self.copy.wait_recv())

    def wait_send(self):
        pl.when(self.sends)(lambda: self.copy.wait_send())


def advect_kernel(rows, nfields, lon, chunks, *refs):
    refs = list(refs)
    fractions_ref, numbers_ref, fields_ref, out_ref, ratio_ref = refs[:5]
    scratch = refs[5:]
    count = len(chunks)
    bufs = []
    for chunk in chunks:
        n = len(buffers_of(chunk[0], rows, 8, LANES))
        bufs.append(scratch[:n])
        scratch = scratch[n:]
    (sums, itab_all, ftab_all, itab, ftab, mass,
     load_sem, bulk_send, bulk_recv, tab_send, tab_recv, tab_local,
     sum_send, sum_recv, mass_send, mass_recv, out_sem) = scratch

    band = lax.axis_index("lat")
    core = lax.axis_index("lev")
    bands = NX * NZ * NY
    y = lax.rem(band, NY)
    z = lax.rem(lax.div(band, NY), NZ)
    x = lax.div(band, NY * NZ)
    base = band - y
    odd = lax.rem(y, 2)
    south = lax.div(y, 2)

    y_up, y_down = lax.rem(y + 1, NY), lax.rem(y + 3, NY)
    y_mates = [(base + lax.rem(y + s, NY), core) for s in (1, 2, 3)]
    z_mates = [(x * (NY * NZ) + lax.rem(z + s, NZ) * NY + y, core) for s in range(1, NZ)]
    x_mates = [(lax.rem(x + s, NX) * (NY * NZ) + z * NY + y, core) for s in range(1, NX)]
    c_mates = [(band, 1 - core)]
    up = (lax.rem(band + NY, bands), core)
    down = (lax.rem(band + bands - NY, bands), core)
    pair = (band + 1 - 2 * odd, core)
    cross = (base + 3 - y, core)
    toward = (lax.rem(band + bands - NY + 2 * NY * south, bands), core)
    diagonal = (lax.rem(base + 3 - y + bands - NY + 2 * NY * south, bands), core)
    outer = jnp.logical_or(y == 0, y == NY - 1)
    inner = jnp.logical_not(outer)
    toward_main = (lax.rem(band + NY + bands - 2 * NY * south, bands), core)
    behind = toward
    before = (lax.rem(band + 1 - 2 * odd + NY + bands - 2 * NY * south, bands), core)
    after = (lax.rem(band + 1 - 2 * odd + bands - NY + 2 * NY * south, bands), core)
    partners = y_mates + z_mates + x_mates + c_mates + [up, down, diagonal, before, after]

    own_at = {"ring": y * rows, "column": rows, "pair": odd * rows, "mirror": south * rows}
    loads = [
        pltpu.make_async_copy(
            fields_ref.at[:, f, :, pl.ds(lane, width)],
            bufs[c][0].at[pl.ds(own_at[scheme], rows)],
            load_sem.at[c],
        )
        for c, (scheme, f, lane, width) in enumerate(chunks)
    ]
    loaded_first = []
    for c in ORDER + list(range(count)):
        if c not in loaded_first:
            loaded_first.append(c)
    for c in loaded_first:
        loads[c].start()

    can_up, can_down = band + NY < bands, band >= NY
    by_half = lambda north, south_side: jnp.logical_or(
        jnp.logical_and(south == 0, north), jnp.logical_and(south == 1, south_side)
    )
    to_up_down, to_down_up = by_half(can_up, can_down), by_half(can_down, can_up)

    barrier = pltpu.get_barrier_semaphore()
    for partner in partners:
        pl.semaphore_signal(barrier, inc=1, device_id=partner, device_id_type=MESH)

    def clear(ref, first, n):
        def one(r, carry):
            ref[first + r] = jnp.zeros(ref.shape[1:], jnp.float32)
            return carry

        lax.fori_loop(0, n, one, 0)

    for at_end, side in ((jnp.logical_not(can_down), 0), (jnp.logical_not(can_up), 1)):

        @pl.when(at_end)
        def _(side=side):
            for b, chunk in zip(bufs, chunks):
                if chunk[0] == "ring":
                    clear(b[3 + side], 0, rows)
                elif chunk[0] == "column":
                    clear(b[0], 2 * side * rows, rows)
                elif chunk[0] == "pair":
                    clear(b[5 + side], 0, rows)
                    pl.when(south == 1 - side)(lambda b=b: clear(b[7], 0, rows))
                else:
                    pl.when(south == side)(lambda b=b: clear(b[5], 0, rows))
                    pl.when(south == side)(lambda b=b: clear(b[7], 0, rows))
                    pl.when(south == 1 - side)(lambda b=b: clear(b[6], 0, rows))

    first_row = band * rows
    low = first_row - numbers_ref[0:1, rows:rows + 1] * rows + 1
    high = first_row + rows - 3 + numbers_ref[0:1, rows + 1:rows + 2] * rows
    start = jnp.minimum(jnp.maximum(numbers_ref[0:1, 0:rows], low), high)
    start = jnp.minimum(jnp.maximum(start, 1), bands * rows - 3) - 1
    lat_w = cubic_weights(fractions_ref[0:1])
    lon_w = cubic_weights(fractions_ref[1:2])
    row_ids = first_row + lax.broadcasted_iota(jnp.int32, (1, rows), 1)
    area = jnp.cos(math.pi * (row_ids.astype(jnp.float32) + 0.5) / (bands * rows) - math.pi / 2.0)
    lon_total = lon_w[0] + lon_w[1] + lon_w[2] + lon_w[3]
    itab_all[0] = jnp.zeros((8, LANES), jnp.int32)
    ftab_all[0] = jnp.zeros((16, LANES), jnp.float32)
    itab_all[0, 0:1, 0:rows] = start
    for k, values in enumerate(lat_w + [area * lon_total] + lon_w + [area]):
        ftab_all[0, k:k + 1, 0:rows] = values

    for load in loads:
        load.wait()

    def row_sums(r, carry):
        pieces = []
        for f in range(nfields):
            total = None
            for c, (scheme, field, lane, width) in enumerate(chunks):
                if field != f:
                    continue
                block = bufs[c][0][own_at[scheme] + r]
                for t in range(width // LANES):
                    tile = block[:, t * LANES:(t + 1) * LANES]
                    total = tile if total is None else total + tile
            pieces.append(jnp.sum(total, axis=0, keepdims=True))
        pieces.append(jnp.zeros((8 - nfields, LANES), jnp.float32))
        sums[y * rows + r] = jnp.concatenate(pieces, axis=0)
        return carry

    lax.fori_loop(0, rows, row_sums, 0)
    pl.semaphore_wait(barrier, len(partners))

    def remote(src, dst, send_sem, recv_sem, target):
        return pltpu.make_async_remote_copy(
            src_ref=src, dst_ref=dst, send_sem=send_sem, recv_sem=recv_sem, device_id=target, device_id_type=MESH
        )

    table_routes = [(2, up), (1, down), (5, y_mates[0]), (4, y_mates[1]), (3, y_mates[2]), (6, diagonal), (7, after)]
    tables = []
    for i, (slot, target) in enumerate(table_routes):
        for j, ref in enumerate((itab_all, ftab_all)):
            tables.append(remote(ref.at[0], ref.at[slot], tab_send.at[2 * i + j], tab_recv.at[2 * i + j], target))
    for copy in tables:
        copy.start()
    my_sums = sums.at[pl.ds(y * rows, rows)]
    sum_copies = [remote(my_sums, my_sums, sum_send.at[s], sum_recv.at[s], y_mates[s]) for s in range(NY - 1)]
    for copy in sum_copies:
        copy.start()

    def ring_spot(row):
        spot = row - base * rows
        return jnp.clip(spot, 0, NY * rows - 1), jnp.logical_and(spot >= 0, spot < NY * rows)

    def pair_spot(row):
        spot = row - (band - odd) * rows
        return jnp.clip(spot, 0, 2 * rows - 1), jnp.logical_and(spot >= 0, spot < 2 * rows)

    mirror_low = (base + jnp.where(outer, 0, 1)) * rows
    mirror_high = (base + jnp.where(outer, 3, 2)) * rows
    mirror_far = (band + NY - 2 * NY * south) * rows

    def mirror_spot(row):
        low_at, high_at = row - mirror_low, row - mirror_high
        in_low = jnp.logical_and(low_at >= 0, low_at < rows)
        in_high = jnp.logical_and(high_at >= 0, high_at < rows)
        spot = jnp.where(in_low, low_at, jnp.clip(high_at, 0, rows - 1) + rows)
        return spot, jnp.logical_or(in_low, in_high)

    def far_spot(row):
        away = row - mirror_far
        return jnp.clip(away, 0, rows - 1), jnp.logical_and(away >= 0, away < rows)

    def column_spot(row):
        away = row - (band - NY) * rows
        block = (away >= NY * rows).astype(jnp.int32) + (away >= 2 * NY * rows).astype(jnp.int32)
        within = away - block * (NY * rows)
        return block * rows + jnp.clip(within, 0, rows - 1), jnp.logical_and(within >= 0, within < rows)

    def taps(spot_of, t, r):
        first = itab[t, 0, r]
        out = []
        for a in range(4):
            spot, inside = spot_of(first + a)
            out.append((spot, jnp.where(inside, ftab[t, a, r], 0.0)))
        return out

    def weighted(ref, spots):
        acc = None
        for spot, weight in spots:
            term = weight * ref[spot]
            acc = term if acc is None else acc + term
        return acc

    def each_row(one):
        def several(i, carry):
            for k in range(UNROLL):
                one(UNROLL * i + k)
            return carry

        lax.fori_loop(0, rows // UNROLL, several, 0)

    def partial_rows(spot_of, src, jobs):
        def one(r):
            for t, dst, extra in jobs:
                acc = weighted(src, taps(spot_of, t, r))
                dst[r] = acc if extra is None else acc + extra[r]

        each_row(one)

    def add_rows(n, dst, dst_at, extra):
        def one(r, carry):
            dst[dst_at + r] = dst[dst_at + r] + extra[r]
            return carry

        lax.fori_loop(0, n, one, 0)

    ready = []

    def need_tables():
        if ready:
            return
        ready.append(True)
        for copy in tables:
            copy.wait_recv()
        moves = [
            pltpu.make_async_copy(itab_all, itab, tab_local.at[0]),
            pltpu.make_async_copy(ftab_all, ftab, tab_local.at[1]),
        ]
        for copy in moves:
            copy.start()
        for copy in moves:
            copy.wait()

    half = rows // 2
    finals = [None] * count

    def stages_of(c):
        scheme = chunks[c][0]
        b = bufs[c]
        send = [bulk_send.at[c, k] for k in range(COPIES[scheme])]
        recv = [bulk_recv.at[c, k] for k in range(COPIES[scheme])]

        def link(k, src, dst, target):
            copy = remote(src, dst, send[k], recv[k], target)
            if target is up:
                return Guarded(copy, can_up, can_down)
            if target is down:
                return Guarded(copy, can_down, can_up)
            if target is toward:
                return Guarded(copy, to_down_up, to_up_down)
            if target is toward_main:
                return Guarded(copy, to_up_down, to_down_up)
            return copy

        if scheme == "ring":
            ring, send_up, send_down, recv_up, recv_down = b
            mine = ring.at[pl.ds(y * rows, rows)]
            from_down = ring.at[pl.ds(y_down * rows + half, rows - half)]
            from_up = ring.at[pl.ds(y_up * rows, half)]
            copies = [
                link(0, mine, mine, y_mates[0]), link(1, mine, mine, y_mates[2]),
                link(2, from_down, from_down, y_mates[0]), link(3, from_up, from_up, y_mates[2]),
                link(4, send_up, recv_up, up), link(5, send_down, recv_down, down),
            ]

            def stage0():
                copies[0].start()
                copies[1].start()

            def stage1():
                copies[0].wait_recv()
                copies[1].wait_recv()
                copies[2].start()
                copies[3].start()

            def stage2():
                copies[2].wait_recv()
                copies[3].wait_recv()
                need_tables()
                partial_rows(ring_spot, ring, [(1, send_up, None), (2, send_down, None)])
                copies[4].start()
                copies[5].start()

            def stage3():
                copies[4].wait_recv()
                copies[5].wait_recv()
                finals[c] = (ring_spot, ring, [recv_up, recv_down], None)

        elif scheme == "column":
            column, to_up, to_down, to_far, far_a, far_b, got_a, got_b = b
            mine = column.at[pl.ds(rows, rows)]
            copies = [
                link(0, mine, column.at[pl.ds(0, rows)], up), link(1, mine, column.at[pl.ds(2 * rows, rows)], down),
                link(2, to_far.at[pl.ds(0, half)], far_a, y_mates[0]),
                link(3, to_far.at[pl.ds(half, rows - half)], far_b, y_mates[2]),
                link(4, to_up, got_a, y_mates[0]), link(5, to_down, got_b, y_mates[2]),
            ]

            def stage0():
                copies[0].start()
                copies[1].start()

            def stage1():
                copies[0].wait_recv()
                copies[1].wait_recv()
                need_tables()
                partial_rows(column_spot, column, [(4, to_far, None)])
                copies[2].start()
                copies[3].start()
                partial_rows(column_spot, column, [(3, to_up, None), (5, to_down, None)])

            def stage2():
                copies[2].wait_recv()
                add_rows(half, to_up, 0, far_a)
                copies[4].start()
                copies[3].wait_recv()
                add_rows(rows - half, to_down, half, far_b)
                copies[5].start()

            def stage3():
                copies[4].wait_recv()
                copies[5].wait_recv()
                finals[c] = (column_spot, column, [got_a, got_b], None)

        elif scheme == "mirror":
            both, to_main, to_behind, to_far, to_cross, from_main, from_behind, passed, from_cross = b
            mine = both.at[pl.ds(south * rows, rows)]
            copies = [
                link(0, mine, mine, cross), link(1, to_main, from_main, toward_main),
                link(2, to_behind, from_behind, behind), link(3, to_far, passed, toward_main),
                link(4, to_cross, from_cross, pair),
            ]
            raw = link(2, mine, from_behind, behind)

            def stage0():
                copies[0].start()
                pl.when(outer)(lambda: raw.start())

            def stage1():
                copies[0].wait_recv()
                need_tables()
                partial_rows(mirror_spot, both, [(7, to_far, None)])
                copies[3].start()
                partial_rows(mirror_spot, both, [(1 + south, to_main, None)])
                copies[1].start()

                @pl.when(inner)
                def _():
                    partial_rows(mirror_spot, both, [(2 - south, to_behind, None)])
                    copies[2].start()

            def stage2():
                copies[3].wait_recv()
                partial_rows(mirror_spot, both, [(3 + 2 * odd, to_cross, passed)])

                @pl.when(outer)
                def _():
                    copies[2].wait_recv()

                    def one(r, carry):
                        to_cross[r] = to_cross[r] + weighted(from_behind, taps(far_spot, 3 + 2 * odd, r))
                        return carry

                    lax.fori_loop(0, rows, one, 0)

                copies[4].start()

            def stage3():
                copies[1].wait_recv()
                copies[4].wait_recv()
                pl.when(inner)(lambda: copies[2].wait_recv())
                finals[c] = (mirror_spot, both, [from_main, from_cross], from_behind)

        else:
            both, to_up, to_down, to_diag, to_cross, from_down, from_up, passed, from_cross = b
            mine = both.at[pl.ds(odd * rows, rows)]
            copies = [
                link(0, mine, mine, pair), link(1, to_up, from_down, up), link(2, to_down, from_up, down),
                link(3, to_diag, passed, toward), link(4, to_cross, from_cross, cross),
            ]

            def stage0():
                copies[0].start()

            def stage1():
                copies[0].wait_recv()
                need_tables()
                partial_rows(pair_spot, both, [(6, to_diag, None)])
                copies[3].start()
                partial_rows(pair_spot, both, [(1, to_up, None), (2, to_down, None)])
                copies[1].start()
                copies[2].start()

            def stage2():
                copies[3].wait_recv()
                partial_rows(pair_spot, both, [(5 - 2 * odd, to_cross, passed)])
                copies[4].start()

            def stage3():
                copies[1].wait_recv()
                copies[2].wait_recv()
                copies[4].wait_recv()
                finals[c] = (pair_spot, both, [from_down, from_up, from_cross], None)

        return copies, [stage0, stage1, stage2, stage3]

    phases = [y_mates, z_mates, c_mates, x_mates]
    offsets = [0]
    for mates in phases:
        offsets.append(offsets[-1] + len(mates))
    mass_copies = []
    for k, mates in enumerate(phases):
        mass_copies.append([
            remote(mass.at[k], mass.at[len(phases) + offsets[k] + i], mass_send.at[offsets[k] + i],
                   mass_recv.at[offsets[k] + i], mate)
            for i, mate in enumerate(mates)
        ])

    def mass_step(step):
        if step == 0:
            need_tables()
            for copy in sum_copies:
                copy.wait_recv()

            def one(r, carry):
                before, after = carry
                before = before + ftab[0, 9, r] * sums[y * rows + r]
                for t in range(3):
                    after = after + ftab[t, 4, r] * weighted(sums, taps(ring_spot, t, r))
                return before, after

            zero = jnp.zeros((8, LANES), jnp.float32)
            before, after = lax.fori_loop(0, rows, one, (zero, zero))
            total = jnp.concatenate([before[0:4], after[0:4]], axis=0)
        else:
            k = step - 1
            total = mass[k]
            for i, copy in enumerate(mass_copies[k]):
                copy.wait_recv()
                total = total + mass[len(phases) + offsets[k] + i]
        if step < len(phases):
            mass[step] = total
            for copy in mass_copies[step]:
                copy.start()
        else:
            total = jnp.sum(total, axis=1, keepdims=True)
            ratio_ref[0:4] = jnp.broadcast_to(total[0:4] / total[4:8], (4, LANES))


    def finish(c):
        _, f, lane, width = chunks[c]
        spot_of, src, extras, far = finals[c]

        def one(r):
            acc = weighted(src, taps(spot_of, 0, r))
            for extra in extras:
                acc = acc + extra[r]
            out_ref[r, f, :, lane:lane + width] = acc

        each_row(one)
        if far is None:
            return

        @pl.when(inner)
        def _():
            def more(r, carry):
                out_ref[r, f, :, lane:lane + width] = out_ref[r, f, :, lane:lane + width] + far[r]
                return carry

            lax.fori_loop(0, rows, more, 0)

        @pl.when(outer)
        def _():
            def more(r, carry):
                acc = weighted(far, taps(far_spot, 0, r))
                out_ref[r, f, :, lane:lane + width] = out_ref[r, f, :, lane:lane + width] + acc
                return carry

            lax.fori_loop(0, rows, more, 0)

    def filter_rows(f):
        def one(r):
            column = out_ref[r, f]
            mixed = ftab[0, 5, r] * column
            for k in range(1, 4):
                mixed = mixed + ftab[0, 5 + k, r] * pltpu.roll(column, lon - k, 1)
            out_ref[r, f] = mixed

        each_row(one)

    every = [stages_of(c) for c in range(count)]
    place = [0] * count
    left = [sum(1 for chunk in chunks if chunk[1] == f) for f in range(nfields)]
    mass_done = 0
    for i, c in enumerate(ORDER):
        every[c][1][place[c]]()
        place[c] += 1
        if place[c] == 4:
            finish(c)
            f = chunks[c][1]
            left[f] -= 1
            if left[f] == 0:
                filter_rows(f)
        while mass_done < len(MASS_AT) and MASS_AT[mass_done] == i:
            mass_step(mass_done)
            mass_done += 1

    for copies, _ in every:
        for copy in copies:
            copy.wait_send()
    for copy in tables + sum_copies:
        copy.wait_send()
    for group in mass_copies:
        for copy in group:
            copy.wait_send()


def turn_kernel(rows, nfields, lon, shift_ref, ratio_ref, column_ref, out_ref, turned_buf, out_sem):
    lane_id = lax.broadcasted_iota(jnp.int32, (8, LANES), 1)
    tiles = lon // LANES
    copies = []
    for step in range(rows // ROWS_PER_STEP):
        at = pl.ds(step * ROWS_PER_STEP, ROWS_PER_STEP)
        copies.append(pltpu.make_async_copy(turned_buf.at[at], out_ref.at[at], out_sem.at[step]))
        for r in range(step * ROWS_PER_STEP, (step + 1) * ROWS_PER_STEP):
            begin = shift_ref[r] - 1
            begin = jnp.where(begin < 0, begin + lon, begin)
            whole = lax.shift_right_logical(begin, 7)
            spots = []
            for t in range(tiles + 1):
                spot = whole + t
                spots.append(pl.multiple_of(jnp.where(spot >= tiles, spot - tiles, spot) * LANES, LANES))
            rest = jnp.bitwise_and(begin, LANES - 1)
            turn = jnp.bitwise_and(LANES - rest, LANES - 1)
            keep = lane_id < (LANES - rest)
            for f in range(nfields):
                ratio = jnp.broadcast_to(ratio_ref[f:f + 1, :], (8, LANES))
                turned = [pltpu.roll(column_ref[r, f, :, pl.ds(spot, LANES)], turn, 1) for spot in spots]
                for t in range(tiles):
                    turned_buf[r, f, :, t * LANES:(t + 1) * LANES] = jnp.where(keep, turned[t], turned[t + 1]) * ratio
        copies[-1].start()
    for copy in copies:
        copy.wait()


def per_device(fields, lat_fraction, lon_fraction, lon_shift, departure_row, extents):
    rows, nfields, levels, lon = fields.shape
    chunks = [(k, f, lane * LANES, width * LANES) for k, f, lane, width in CHUNKS]
    count = len(chunks)
    dma = pltpu.SemaphoreType.DMA
    mates = (NX - 1) + 1 + (NZ - 1) + (NY - 1)
    scratch = []
    for scheme, _, _, width in chunks:
        scratch += buffers_of(scheme, rows, levels, width)
    scratch += [
        pltpu.VMEM((NY * rows, 8, LANES), jnp.float32),
        pltpu.VMEM((8, 8, LANES), jnp.int32),
        pltpu.VMEM((8, 16, LANES), jnp.float32),
        pltpu.SMEM((8, 8, LANES), jnp.int32),
        pltpu.SMEM((8, 16, LANES), jnp.float32),
        pltpu.VMEM((4 + mates, 8, LANES), jnp.float32),
        dma((count,)), dma((count, 6)), dma((count, 6)), dma((14,)), dma((14,)), dma((2,)),
        dma((NY - 1,)), dma((NY - 1,)), dma((mates,)), dma((mates,)), dma((nfields,)),
    ]
    vmem = pl.BlockSpec(memory_space=pltpu.VMEM)
    column, ratio = pl.pallas_call(
        functools.partial(advect_kernel, rows, nfields, lon, chunks),
        out_shape=(
            jax.ShapeDtypeStruct(fields.shape, fields.dtype),
            jax.ShapeDtypeStruct((4, LANES), jnp.float32),
        ),
        in_specs=[vmem, vmem, pl.BlockSpec(memory_space=pl.ANY)],
        out_specs=(vmem, vmem),
        scratch_shapes=scratch,
        compiler_params=pltpu.CompilerParams(collective_id=0, has_side_effects=True, vmem_limit_bytes=KERNEL_VMEM),
    )(jnp.stack([lat_fraction, lon_fraction]), jnp.concatenate([departure_row[None], extents], axis=1), fields)
    return pl.pallas_call(
        functools.partial(turn_kernel, rows, nfields, lon),
        out_shape=jax.ShapeDtypeStruct(fields.shape, fields.dtype),
        in_specs=[pl.BlockSpec(memory_space=pltpu.SMEM), vmem, vmem],
        out_specs=pl.BlockSpec(memory_space=pl.ANY),
        scratch_shapes=[pltpu.VMEM(fields.shape, fields.dtype), dma((rows // ROWS_PER_STEP,))],
        compiler_params=pltpu.CompilerParams(vmem_limit_bytes=16 * 1024 * 1024),
    )(lon_shift, ratio, column)


def solution(mesh):
    placed = (P("lat", None, "lev", None), P("lat"), P("lat"), P("lat"), P("lat"), P("lat", None))
    return jax.shard_map(
        per_device,
        mesh=mesh,
        in_specs=placed,
        out_specs=P("lat", None, "lev", None),
        check_vma=False,
    )
```

```python
import functools
import math

import jax
import jax.numpy as jnp
from jax import lax
from jax.experimental import pallas as pl
from jax.experimental.pallas import tpu as pltpu
from jax.sharding import PartitionSpec as P

MESH = pl.DeviceIdType.MESH
NY, NZ, NX = 4, 8, 4
LANES = 128
ROWS_PER_STEP = 1
UNROLL = 2
KERNEL_VMEM = 50 * 1024 * 1024
CHUNKS = [('column', 0, 0, 10), ('mirror', 0, 10, 10), ('ring', 1, 0, 15), ('column', 1, 15, 5), ('mirror', 2, 0, 5), ('pair', 2, 5, 15)]
ORDER = [0, 4, 5, 1, 2, 3, 4, 0, 5, 1, 2, 0, 3, 5, 1, 2, 0, 4, 3, 1, 4, 5, 2, 3]
MASS_AT = [2, 8, 18, 18, 23]


def cubic_weights(fraction):
    return [
        -fraction * (fraction - 1.0) * (fraction - 2.0) / 6.0,
        (fraction + 1.0) * (fraction - 1.0) * (fraction - 2.0) / 2.0,
        -(fraction + 1.0) * fraction * (fraction - 2.0) / 2.0,
        (fraction + 1.0) * fraction * (fraction - 1.0) / 6.0,
    ]


def buffers_of(scheme, rows, levels, width):
    half = rows // 2
    counts = {
        "ring": [NY * rows] + [rows] * 4,
        "column": [3 * rows] + [rows] * 3 + [half, rows - half] + [rows] * 2,
        "pair": [2 * rows] + [rows] * 8,
        "mirror": [2 * rows] + [rows] * 8,
    }[scheme]
    return [pltpu.VMEM((n, levels, width), jnp.float32) for n in counts]


COPIES = {"ring": 6, "column": 6, "pair": 5, "mirror": 5}


class Guarded:
    def __init__(self, copy, sends, gets):
        self.copy, self.sends, self.gets = copy, sends, gets

    def start(self):
        pl.when(self.sends)(lambda: self.copy.start())

    def wait_recv(self):
        pl.when(self.gets)(lambda: self.copy.wait_recv())

    def wait_send(self):
        pl.when(self.sends)(lambda: self.copy.wait_send())


def advect_kernel(rows, nfields, lon, chunks, *refs):
    refs = list(refs)
    fractions_ref, numbers_ref, fields_ref, out_ref, ratio_ref = refs[:5]
    scratch = refs[5:]
    count = len(chunks)
    bufs = []
    for chunk in chunks:
        n = len(buffers_of(chunk[0], rows, 8, LANES))
        bufs.append(scratch[:n])
        scratch = scratch[n:]
    (sums, itab_all, ftab_all, itab, ftab, mass,
     load_sem, bulk_send, bulk_recv, tab_send, tab_recv, tab_local,
     sum_send, sum_recv, mass_send, mass_recv, out_sem) = scratch

    band = lax.axis_index("lat")
    core = lax.axis_index("lev")
    bands = NX * NZ * NY
    y = lax.rem(band, NY)
    z = lax.rem(lax.div(band, NY), NZ)
    x = lax.div(band, NY * NZ)
    base = band - y
    odd = lax.rem(y, 2)
    south = lax.div(y, 2)

    y_up, y_down = lax.rem(y + 1, NY), lax.rem(y + 3, NY)
    y_mates = [(base + lax.rem(y + s, NY), core) for s in (1, 2, 3)]
    z_mates = [(x * (NY * NZ) + lax.rem(z + s, NZ) * NY + y, core) for s in range(1, NZ)]
    x_mates = [(lax.rem(x + s, NX) * (NY * NZ) + z * NY + y, core) for s in range(1, NX)]
    c_mates = [(band, 1 - core)]
    up = (lax.rem(band + NY, bands), core)
    down = (lax.rem(band + bands - NY, bands), core)
    pair = (band + 1 - 2 * odd, core)
    cross = (base + 3 - y, core)
    toward = (lax.rem(band + bands - NY + 2 * NY * south, bands), core)
    diagonal = (lax.rem(base + 3 - y + bands - NY + 2 * NY * south, bands), core)
    outer = jnp.logical_or(y == 0, y == NY - 1)
    inner = jnp.logical_not(outer)
    toward_main = (lax.rem(band + NY + bands - 2 * NY * south, bands), core)
    behind = toward
    before = (lax.rem(band + 1 - 2 * odd + NY + bands - 2 * NY * south, bands), core)
    after = (lax.rem(band + 1 - 2 * odd + bands - NY + 2 * NY * south, bands), core)
    partners = y_mates + z_mates + x_mates + c_mates + [up, down, diagonal, before, after]

    own_at = {"ring": y * rows, "column": rows, "pair": odd * rows, "mirror": south * rows}
    loads = [
        pltpu.make_async_copy(
            fields_ref.at[:, f, :, pl.ds(lane, width)],
            bufs[c][0].at[pl.ds(own_at[scheme], rows)],
            load_sem.at[c],
        )
        for c, (scheme, f, lane, width) in enumerate(chunks)
    ]
    loaded_first = []
    for c in ORDER + list(range(count)):
        if c not in loaded_first:
            loaded_first.append(c)
    for c in loaded_first:
        loads[c].start()

    can_up, can_down = band + NY < bands, band >= NY
    by_half = lambda north, south_side: jnp.logical_or(
        jnp.logical_and(south == 0, north), jnp.logical_and(south == 1, south_side)
    )
    to_up_down, to_down_up = by_half(can_up, can_down), by_half(can_down, can_up)

    barrier = pltpu.get_barrier_semaphore()
    for partner in partners:
        pl.semaphore_signal(barrier, inc=1, device_id=partner, device_id_type=MESH)

    def clear(ref, first, n):
        def one(r, carry):
            ref[first + r] = jnp.zeros(ref.shape[1:], jnp.float32)
            return carry

        lax.fori_loop(0, n, one, 0)

    for at_end, side in ((jnp.logical_not(can_down), 0), (jnp.logical_not(can_up), 1)):

        @pl.when(at_end)
        def _(side=side):
            for b, chunk in zip(bufs, chunks):
                if chunk[0] == "ring":
                    clear(b[3 + side], 0, rows)
                elif chunk[0] == "column":
                    clear(b[0], 2 * side * rows, rows)
                elif chunk[0] == "pair":
                    clear(b[5 + side], 0, rows)
                    pl.when(south == 1 - side)(lambda b=b: clear(b[7], 0, rows))
                else:
                    pl.when(south == side)(lambda b=b: clear(b[5], 0, rows))
                    pl.when(south == side)(lambda b=b: clear(b[7], 0, rows))
                    pl.when(south == 1 - side)(lambda b=b: clear(b[6], 0, rows))

    first_row = band * rows
    low = first_row - numbers_ref[0:1, rows:rows + 1] * rows + 1
    high = first_row + rows - 3 + numbers_ref[0:1, rows + 1:rows + 2] * rows
    start = jnp.minimum(jnp.maximum(numbers_ref[0:1, 0:rows], low), high)
    start = jnp.minimum(jnp.maximum(start, 1), bands * rows - 3) - 1
    lat_w = cubic_weights(fractions_ref[0:1])
    lon_w = cubic_weights(fractions_ref[1:2])
    row_ids = first_row + lax.broadcasted_iota(jnp.int32, (1, rows), 1)
    area = jnp.cos(math.pi * (row_ids.astype(jnp.float32) + 0.5) / (bands * rows) - math.pi / 2.0)
    lon_total = lon_w[0] + lon_w[1] + lon_w[2] + lon_w[3]
    itab_all[0] = jnp.zeros((8, LANES), jnp.int32)
    ftab_all[0] = jnp.zeros((16, LANES), jnp.float32)
    itab_all[0, 0:1, 0:rows] = start
    for k, values in enumerate(lat_w + [area * lon_total] + lon_w + [area]):
        ftab_all[0, k:k + 1, 0:rows] = values

    def row_sums(r, carry):
        pieces = []
        for f in range(nfields):
            total = None
            for c, (scheme, field, lane, width) in enumerate(chunks):
                if field != f:
                    continue
                block = bufs[c][0][own_at[scheme] + r]
                for t in range(width // LANES):
                    tile = block[:, t * LANES:(t + 1) * LANES]
                    total = tile if total is None else total + tile
            pieces.append(jnp.sum(total, axis=0, keepdims=True))
        pieces.append(jnp.zeros((8 - nfields, LANES), jnp.float32))
        sums[y * rows + r] = jnp.concatenate(pieces, axis=0)
        return carry

    pl.semaphore_wait(barrier, len(partners))

    def remote(src, dst, send_sem, recv_sem, target):
        return pltpu.make_async_remote_copy(
            src_ref=src, dst_ref=dst, send_sem=send_sem, recv_sem=recv_sem, device_id=target, device_id_type=MESH
        )

    table_routes = [(2, up), (1, down), (5, y_mates[0]), (4, y_mates[1]), (3, y_mates[2]), (6, diagonal), (7, after)]
    tables = []
    for i, (slot, target) in enumerate(table_routes):
        for j, ref in enumerate((itab_all, ftab_all)):
            tables.append(remote(ref.at[0], ref.at[slot], tab_send.at[2 * i + j], tab_recv.at[2 * i + j], target))
    for copy in tables:
        copy.start()
    my_sums = sums.at[pl.ds(y * rows, rows)]
    sum_copies = [remote(my_sums, my_sums, sum_send.at[s], sum_recv.at[s], y_mates[s]) for s in range(NY - 1)]
    def ring_spot(row):
        spot = row - base * rows
        return jnp.clip(spot, 0, NY * rows - 1), jnp.logical_and(spot >= 0, spot < NY * rows)

    def pair_spot(row):
        spot = row - (band - odd) * rows
        return jnp.clip(spot, 0, 2 * rows - 1), jnp.logical_and(spot >= 0, spot < 2 * rows)

    mirror_low = (base + jnp.where(outer, 0, 1)) * rows
    mirror_high = (base + jnp.where(outer, 3, 2)) * rows
    mirror_far = (band + NY - 2 * NY * south) * rows

    def mirror_spot(row):
        low_at, high_at = row - mirror_low, row - mirror_high
        in_low = jnp.logical_and(low_at >= 0, low_at < rows)
        in_high = jnp.logical_and(high_at >= 0, high_at < rows)
        spot = jnp.where(in_low, low_at, jnp.clip(high_at, 0, rows - 1) + rows)
        return spot, jnp.logical_or(in_low, in_high)

    def far_spot(row):
        away = row - mirror_far
        return jnp.clip(away, 0, rows - 1), jnp.logical_and(away >= 0, away < rows)

    def column_spot(row):
        away = row - (band - NY) * rows
        block = (away >= NY * rows).astype(jnp.int32) + (away >= 2 * NY * rows).astype(jnp.int32)
        within = away - block * (NY * rows)
        return block * rows + jnp.clip(within, 0, rows - 1), jnp.logical_and(within >= 0, within < rows)

    def taps(spot_of, t, r):
        first = itab[t, 0, r]
        out = []
        for a in range(4):
            spot, inside = spot_of(first + a)
            out.append((spot, jnp.where(inside, ftab[t, a, r], 0.0)))
        return out

    def weighted(ref, spots):
        acc = None
        for spot, weight in spots:
            term = weight * ref[spot]
            acc = term if acc is None else acc + term
        return acc

    def each_row(one):
        def several(i, carry):
            for k in range(UNROLL):
                one(UNROLL * i + k)
            return carry

        lax.fori_loop(0, rows // UNROLL, several, 0)

    def partial_rows(spot_of, src, jobs):
        def one(r):
            for t, dst, extra in jobs:
                acc = weighted(src, taps(spot_of, t, r))
                dst[r] = acc if extra is None else acc + extra[r]

        each_row(one)

    def add_rows(n, dst, dst_at, extra):
        def one(r, carry):
            dst[dst_at + r] = dst[dst_at + r] + extra[r]
            return carry

        lax.fori_loop(0, n, one, 0)

    ready = []

    def need_tables():
        if ready:
            return
        ready.append(True)
        for copy in tables:
            copy.wait_recv()
        moves = [
            pltpu.make_async_copy(itab_all, itab, tab_local.at[0]),
            pltpu.make_async_copy(ftab_all, ftab, tab_local.at[1]),
        ]
        for copy in moves:
            copy.start()
        for copy in moves:
            copy.wait()

    half = rows // 2
    finals = [None] * count

    def stages_of(c):
        scheme = chunks[c][0]
        b = bufs[c]
        send = [bulk_send.at[c, k] for k in range(COPIES[scheme])]
        recv = [bulk_recv.at[c, k] for k in range(COPIES[scheme])]

        def link(k, src, dst, target):
            copy = remote(src, dst, send[k], recv[k], target)
            if target is up:
                return Guarded(copy, can_up, can_down)
            if target is down:
                return Guarded(copy, can_down, can_up)
            if target is toward:
                return Guarded(copy, to_down_up, to_up_down)
            if target is toward_main:
                return Guarded(copy, to_up_down, to_down_up)
            return copy

        if scheme == "ring":
            ring, send_up, send_down, recv_up, recv_down = b
            mine = ring.at[pl.ds(y * rows, rows)]
            from_down = ring.at[pl.ds(y_down * rows + half, rows - half)]
            from_up = ring.at[pl.ds(y_up * rows, half)]
            copies = [
                link(0, mine, mine, y_mates[0]), link(1, mine, mine, y_mates[2]),
                link(2, from_down, from_down, y_mates[0]), link(3, from_up, from_up, y_mates[2]),
                link(4, send_up, recv_up, up), link(5, send_down, recv_down, down),
            ]

            def stage0():
                copies[0].start()
                copies[1].start()

            def stage1():
                copies[0].wait_recv()
                copies[1].wait_recv()
                copies[2].start()
                copies[3].start()

            def stage2():
                copies[2].wait_recv()
                copies[3].wait_recv()
                need_tables()
                partial_rows(ring_spot, ring, [(1, send_up, None), (2, send_down, None)])
                copies[4].start()
                copies[5].start()

            def stage3():
                copies[4].wait_recv()
                copies[5].wait_recv()
                finals[c] = (ring_spot, ring, [recv_up, recv_down], None)

        elif scheme == "column":
            column, to_up, to_down, to_far, far_a, far_b, got_a, got_b = b
            mine = column.at[pl.ds(rows, rows)]
            copies = [
                link(0, mine, column.at[pl.ds(0, rows)], up), link(1, mine, column.at[pl.ds(2 * rows, rows)], down),
                link(2, to_far.at[pl.ds(0, half)], far_a, y_mates[0]),
                link(3, to_far.at[pl.ds(half, rows - half)], far_b, y_mates[2]),
                link(4, to_up, got_a, y_mates[0]), link(5, to_down, got_b, y_mates[2]),
            ]

            def stage0():
                copies[0].start()
                copies[1].start()

            def stage1():
                copies[0].wait_recv()
                copies[1].wait_recv()
                need_tables()
                partial_rows(column_spot, column, [(4, to_far, None)])
                copies[2].start()
                copies[3].start()
                partial_rows(column_spot, column, [(3, to_up, None), (5, to_down, None)])

            def stage2():
                copies[2].wait_recv()
                add_rows(half, to_up, 0, far_a)
                copies[4].start()
                copies[3].wait_recv()
                add_rows(rows - half, to_down, half, far_b)
                copies[5].start()

            def stage3():
                copies[4].wait_recv()
                copies[5].wait_recv()
                finals[c] = (column_spot, column, [got_a, got_b], None)

        elif scheme == "mirror":
            both, to_main, to_behind, to_far, to_cross, from_main, from_behind, passed, from_cross = b
            mine = both.at[pl.ds(south * rows, rows)]
            copies = [
                link(0, mine, mine, cross), link(1, to_main, from_main, toward_main),
                link(2, to_behind, from_behind, behind), link(3, to_far, passed, toward_main),
                link(4, to_cross, from_cross, pair),
            ]
            raw = link(2, mine, from_behind, behind)

            def stage0():
                copies[0].start()
                pl.when(outer)(lambda: raw.start())

            def stage1():
                copies[0].wait_recv()
                need_tables()
                partial_rows(mirror_spot, both, [(7, to_far, None)])
                copies[3].start()
                partial_rows(mirror_spot, both, [(1 + south, to_main, None)])
                copies[1].start()

                @pl.when(inner)
                def _():
                    partial_rows(mirror_spot, both, [(2 - south, to_behind, None)])
                    copies[2].start()

            def stage2():
                copies[3].wait_recv()
                partial_rows(mirror_spot, both, [(3 + 2 * odd, to_cross, passed)])

                @pl.when(outer)
                def _():
                    copies[2].wait_recv()

                    def one(r, carry):
                        to_cross[r] = to_cross[r] + weighted(from_behind, taps(far_spot, 3 + 2 * odd, r))
                        return carry

                    lax.fori_loop(0, rows, one, 0)

                copies[4].start()

            def stage3():
                copies[1].wait_recv()
                copies[4].wait_recv()
                pl.when(inner)(lambda: copies[2].wait_recv())
                finals[c] = (mirror_spot, both, [from_main, from_cross], from_behind)

        else:
            both, to_up, to_down, to_diag, to_cross, from_down, from_up, passed, from_cross = b
            mine = both.at[pl.ds(odd * rows, rows)]
            copies = [
                link(0, mine, mine, pair), link(1, to_up, from_down, up), link(2, to_down, from_up, down),
                link(3, to_diag, passed, toward), link(4, to_cross, from_cross, cross),
            ]

            def stage0():
                copies[0].start()

            def stage1():
                copies[0].wait_recv()
                need_tables()
                partial_rows(pair_spot, both, [(6, to_diag, None)])
                copies[3].start()
                partial_rows(pair_spot, both, [(1, to_up, None), (2, to_down, None)])
                copies[1].start()
                copies[2].start()

            def stage2():
                copies[3].wait_recv()
                partial_rows(pair_spot, both, [(5 - 2 * odd, to_cross, passed)])
                copies[4].start()

            def stage3():
                copies[1].wait_recv()
                copies[2].wait_recv()
                copies[4].wait_recv()
                finals[c] = (pair_spot, both, [from_down, from_up, from_cross], None)

        return copies, [stage0, stage1, stage2, stage3]

    phases = [y_mates, z_mates, c_mates, x_mates]
    offsets = [0]
    for mates in phases:
        offsets.append(offsets[-1] + len(mates))
    mass_copies = []
    for k, mates in enumerate(phases):
        mass_copies.append([
            remote(mass.at[k], mass.at[len(phases) + offsets[k] + i], mass_send.at[offsets[k] + i],
                   mass_recv.at[offsets[k] + i], mate)
            for i, mate in enumerate(mates)
        ])

    def mass_step(step):
        if step == 0:
            need_tables()
            for copy in sum_copies:
                copy.wait_recv()

            def one(r, carry):
                before, after = carry
                before = before + ftab[0, 9, r] * sums[y * rows + r]
                for t in range(3):
                    after = after + ftab[t, 4, r] * weighted(sums, taps(ring_spot, t, r))
                return before, after

            zero = jnp.zeros((8, LANES), jnp.float32)
            before, after = lax.fori_loop(0, rows, one, (zero, zero))
            total = jnp.concatenate([before[0:4], after[0:4]], axis=0)
        else:
            k = step - 1
            total = mass[k]
            for i, copy in enumerate(mass_copies[k]):
                copy.wait_recv()
                total = total + mass[len(phases) + offsets[k] + i]
        if step < len(phases):
            mass[step] = total
            for copy in mass_copies[step]:
                copy.start()
        else:
            total = jnp.sum(total, axis=1, keepdims=True)
            ratio_ref[0:4] = jnp.broadcast_to(total[0:4] / total[4:8], (4, LANES))


    def finish(c):
        _, f, lane, width = chunks[c]
        spot_of, src, extras, far = finals[c]

        def one(r):
            acc = weighted(src, taps(spot_of, 0, r))
            for extra in extras:
                acc = acc + extra[r]
            out_ref[r, f, :, lane:lane + width] = acc

        each_row(one)
        if far is None:
            return

        @pl.when(inner)
        def _():
            def more(r, carry):
                out_ref[r, f, :, lane:lane + width] = out_ref[r, f, :, lane:lane + width] + far[r]
                return carry

            lax.fori_loop(0, rows, more, 0)

        @pl.when(outer)
        def _():
            def more(r, carry):
                acc = weighted(far, taps(far_spot, 0, r))
                out_ref[r, f, :, lane:lane + width] = out_ref[r, f, :, lane:lane + width] + acc
                return carry

            lax.fori_loop(0, rows, more, 0)

    def filter_rows(f):
        def one(r):
            column = out_ref[r, f]
            mixed = ftab[0, 5, r] * column
            for k in range(1, 4):
                mixed = mixed + ftab[0, 5 + k, r] * pltpu.roll(column, lon - k, 1)
            out_ref[r, f] = mixed

        each_row(one)

    every = [stages_of(c) for c in range(count)]
    place = [0] * count
    left = [sum(1 for chunk in chunks if chunk[1] == f) for f in range(nfields)]
    mass_done = 0
    for i, c in enumerate(ORDER):
        if i == 0:
            loads[c].wait()
        if i == 1:
            for other in range(count):
                if other != ORDER[0]:
                    loads[other].wait()
            lax.fori_loop(0, rows, row_sums, 0)
            for copy in sum_copies:
                copy.start()
        every[c][1][place[c]]()
        place[c] += 1
        if place[c] == 4:
            finish(c)
            f = chunks[c][1]
            left[f] -= 1
            if left[f] == 0:
                filter_rows(f)
        while mass_done < len(MASS_AT) and MASS_AT[mass_done] == i:
            mass_step(mass_done)
            mass_done += 1

    for copies, _ in every:
        for copy in copies:
            copy.wait_send()
    for copy in tables + sum_copies:
        copy.wait_send()
    for group in mass_copies:
        for copy in group:
            copy.wait_send()


def turn_kernel(rows, nfields, lon, shift_ref, ratio_ref, column_ref, out_ref, turned_buf, out_sem):
    lane_id = lax.broadcasted_iota(jnp.int32, (8, LANES), 1)
    tiles = lon // LANES
    copies = []
    for step in range(rows // ROWS_PER_STEP):
        at = pl.ds(step * ROWS_PER_STEP, ROWS_PER_STEP)
        copies.append(pltpu.make_async_copy(turned_buf.at[at], out_ref.at[at], out_sem.at[step]))
        for r in range(step * ROWS_PER_STEP, (step + 1) * ROWS_PER_STEP):
            begin = shift_ref[r] - 1
            begin = jnp.where(begin < 0, begin + lon, begin)
            whole = lax.shift_right_logical(begin, 7)
            spots = []
            for t in range(tiles + 1):
                spot = whole + t
                spots.append(pl.multiple_of(jnp.where(spot >= tiles, spot - tiles, spot) * LANES, LANES))
            rest = jnp.bitwise_and(begin, LANES - 1)
            turn = jnp.bitwise_and(LANES - rest, LANES - 1)
            keep = lane_id < (LANES - rest)
            for f in range(nfields):
                ratio = jnp.broadcast_to(ratio_ref[f:f + 1, :], (8, LANES))
                turned = [pltpu.roll(column_ref[r, f, :, pl.ds(spot, LANES)], turn, 1) for spot in spots]
                for t in range(tiles):
                    turned_buf[r, f, :, t * LANES:(t + 1) * LANES] = jnp.where(keep, turned[t], turned[t + 1]) * ratio
        copies[-1].start()
    for copy in copies:
        copy.wait()


def per_device(fields, lat_fraction, lon_fraction, lon_shift, departure_row, extents):
    rows, nfields, levels, lon = fields.shape
    chunks = [(k, f, lane * LANES, width * LANES) for k, f, lane, width in CHUNKS]
    count = len(chunks)
    dma = pltpu.SemaphoreType.DMA
    mates = (NX - 1) + 1 + (NZ - 1) + (NY - 1)
    scratch = []
    for scheme, _, _, width in chunks:
        scratch += buffers_of(scheme, rows, levels, width)
    scratch += [
        pltpu.VMEM((NY * rows, 8, LANES), jnp.float32),
        pltpu.VMEM((8, 8, LANES), jnp.int32),
        pltpu.VMEM((8, 16, LANES), jnp.float32),
        pltpu.SMEM((8, 8, LANES), jnp.int32),
        pltpu.SMEM((8, 16, LANES), jnp.float32),
        pltpu.VMEM((4 + mates, 8, LANES), jnp.float32),
        dma((count,)), dma((count, 6)), dma((count, 6)), dma((14,)), dma((14,)), dma((2,)),
        dma((NY - 1,)), dma((NY - 1,)), dma((mates,)), dma((mates,)), dma((nfields,)),
    ]
    vmem = pl.BlockSpec(memory_space=pltpu.VMEM)
    column, ratio = pl.pallas_call(
        functools.partial(advect_kernel, rows, nfields, lon, chunks),
        out_shape=(
            jax.ShapeDtypeStruct(fields.shape, fields.dtype),
            jax.ShapeDtypeStruct((4, LANES), jnp.float32),
        ),
        in_specs=[vmem, vmem, pl.BlockSpec(memory_space=pl.ANY)],
        out_specs=(vmem, vmem),
        scratch_shapes=scratch,
        compiler_params=pltpu.CompilerParams(collective_id=0, has_side_effects=True, vmem_limit_bytes=KERNEL_VMEM),
    )(jnp.stack([lat_fraction, lon_fraction]), jnp.concatenate([departure_row[None], extents], axis=1), fields)
    return pl.pallas_call(
        functools.partial(turn_kernel, rows, nfields, lon),
        out_shape=jax.ShapeDtypeStruct(fields.shape, fields.dtype),
        in_specs=[pl.BlockSpec(memory_space=pltpu.SMEM), vmem, vmem],
        out_specs=pl.BlockSpec(memory_space=pl.ANY),
        scratch_shapes=[pltpu.VMEM(fields.shape, fields.dtype), dma((rows // ROWS_PER_STEP,))],
        compiler_params=pltpu.CompilerParams(vmem_limit_bytes=16 * 1024 * 1024),
    )(lon_shift, ratio, column)


def solution(mesh):
    placed = (P("lat", None, "lev", None), P("lat"), P("lat"), P("lat"), P("lat"), P("lat", None))
    return jax.shard_map(
        per_device,
        mesh=mesh,
        in_specs=placed,
        out_specs=P("lat", None, "lev", None),
        check_vma=False,
    )
```
